32 devices in a mesh: dp: 1 (over z), tp: 4 (over y), ep: 8 (over x, core).
Axes of the slice: x: 4, y: 4, z: 1, core: 2. Of those that a mesh axis runs over, the one named last changes fastest.
The devices are a block of a 4x4x8 slice.
Arguments:
- x_tok: bfloat16 [8192, 768], P(('dp', 'ep'))
- w_router: float32 [768, 64], replicated
- w_gelu: bfloat16 [64, 768, 3072], P('ep', None, 'tp')
- w_lin: bfloat16 [64, 768, 3072], P('ep', None, 'tp')
- w_out: bfloat16 [64, 3072, 768], P('ep', 'tp')
- expert_idx: int32 [8192, 2], P(('dp', 'ep'))
- slot_idx: int32 [8192, 2], P(('dp', 'ep'))
Outputs:
- output: bfloat16 [8192, 768], P(('dp', 'ep'))
All inputs are finite; a program needn't handle non-finite values.
Results may differ from the reference program's by a relative error of at most 0.0115141.
Values are sent between devices in bfloat16 or wider.
A program may use at most 768 MiB of HBM per device.

```python
import jax
import jax.numpy as jnp
from jax import lax

D_MODEL = 768
D_FF = 3072
EXPERTS = 64
EP_GROUPS = 8
TOK_SHARD = 1024
CAP_LOCAL = 64
NUM_TOKENS = EP_GROUPS * TOK_SHARD
CAPACITY = EP_GROUPS * CAP_LOCAL


def draw_routing(route_key):
    k_perm, k_first, k_second = jax.random.split(route_key, 3)
    expert_order = jax.random.permutation(k_perm, EXPERTS)
    rank_draws = jax.random.randint(k_first, (2, EP_GROUPS, TOK_SHARD), 0, EXPERTS)
    first_rank = jnp.minimum(rank_draws[0], rank_draws[1])
    tok_pos = jnp.arange(TOK_SHARD)[None, :]
    first_rank = jnp.where(tok_pos < CAP_LOCAL, 0, first_rank)
    first_choice = expert_order[first_rank]
    offset = jax.random.randint(k_second, (EP_GROUPS, TOK_SHARD), 1, EXPERTS)
    second_choice = (first_choice + offset) % EXPERTS
    choices = jnp.stack([first_choice, second_choice], axis=1)
    onehot = (choices[..., None] == jnp.arange(EXPERTS)).astype(jnp.int32)
    flat_hot = onehot.reshape(EP_GROUPS, 2 * TOK_SHARD, EXPERTS)
    before = jnp.cumsum(flat_hot, axis=1) - flat_hot
    position = jnp.sum(before * flat_hot, axis=2).reshape(EP_GROUPS, 2, TOK_SHARD)
    slot_base = (jnp.arange(EP_GROUPS) * CAP_LOCAL)[:, None, None]
    slot_table = jnp.where(position < CAP_LOCAL, slot_base + position, -1)
    expert_idx = jnp.transpose(choices, (0, 2, 1)).reshape(NUM_TOKENS, 2)
    slot_idx = jnp.transpose(slot_table, (0, 2, 1)).reshape(NUM_TOKENS, 2)
    return expert_idx.astype(jnp.int32), slot_idx.astype(jnp.int32)


def setup_inputs(seed: int = 0, part: int = 0) -> dict:
    part_key = jax.random.fold_in(jax.random.key(seed), part)
    k_tok, k_route = jax.random.split(part_key, 2)
    k_router, k_gelu, k_lin, k_out = jax.random.split(jax.random.key(seed + 1), 4)
    x_tok = jax.random.normal(k_tok, (NUM_TOKENS, D_MODEL), jnp.float32).astype(jnp.bfloat16)
    w_router = 1.5 * D_MODEL ** -0.5 * jax.random.normal(k_router, (D_MODEL, EXPERTS), jnp.float32)
    w_gelu = (D_MODEL ** -0.5 * jax.random.normal(k_gelu, (EXPERTS, D_MODEL, D_FF), jnp.float32)).astype(jnp.bfloat16)
    w_lin = (D_MODEL ** -0.5 * jax.random.normal(k_lin, (EXPERTS, D_MODEL, D_FF), jnp.float32)).astype(jnp.bfloat16)
    w_out = (D_FF ** -0.5 * jax.random.normal(k_out, (EXPERTS, D_FF, D_MODEL), jnp.float32)).astype(jnp.bfloat16)
    expert_idx, slot_idx = draw_routing(k_route)
    return {"x_tok": x_tok, "w_router": w_router, "w_gelu": w_gelu, "w_lin": w_lin, "w_out": w_out, "expert_idx": expert_idx, "slot_idx": slot_idx}


def expert_ffn(expert_args):
    expert_rows, w_gelu_e, w_lin_e, w_out_e = expert_args
    gate_pre = jnp.dot(expert_rows, w_gelu_e, preferred_element_type=jnp.float32)
    lin_pre = jnp.dot(expert_rows, w_lin_e, preferred_element_type=jnp.float32)
    hidden = (jax.nn.gelu(gate_pre, approximate=True) * lin_pre).astype(jnp.bfloat16)
    return jnp.dot(hidden, w_out_e, preferred_element_type=jnp.float32).astype(jnp.bfloat16)


def reference(x_tok, w_router, w_gelu, w_lin, w_out, expert_idx, slot_idx):
    logits = jnp.dot(x_tok.astype(jnp.float32), w_router)
    router_prob = jax.nn.softmax(logits, axis=-1)
    picked = jnp.take_along_axis(router_prob, expert_idx, axis=1)
    gate_val = picked / jnp.sum(picked, axis=1, keepdims=True)
    dest_row = jnp.where(slot_idx >= 0, expert_idx * CAPACITY + slot_idx, EXPERTS * CAPACITY)
    token_ids = jnp.broadcast_to(jnp.arange(NUM_TOKENS, dtype=jnp.int32)[:, None], (NUM_TOKENS, 2))
    source = jnp.full((EXPERTS * CAPACITY,), NUM_TOKENS, jnp.int32).at[dest_row.reshape(-1)].set(token_ids.reshape(-1), mode="drop")
    buffers = jnp.take(x_tok, source, axis=0, mode="fill", fill_value=0).reshape(EXPERTS, CAPACITY, D_MODEL)
    expert_out = lax.map(expert_ffn, (buffers, w_gelu, w_lin, w_out))
    back_rows = jnp.take(expert_out.reshape(EXPERTS * CAPACITY, D_MODEL), dest_row, axis=0, mode="fill", fill_value=0)
    combined = jnp.sum(gate_val[:, :, None] * back_rows.astype(jnp.float32), axis=1)
    return combined.astype(jnp.bfloat16)
```

```python
import functools

import jax
import jax.numpy as jnp
from jax import lax
from jax.experimental import pallas as pl
from jax.experimental.pallas import tpu as pltpu
from jax.sharding import PartitionSpec as P

CAP_FACTOR = 2
LANES = 128
MESH = pl.DeviceIdType.MESH
F32 = jnp.float32
BF16 = jnp.bfloat16
UNITS = [(0, 0), (0, 1), (1, 0), (0, 2), (0, 3), (1, 1), (0, 4), (1, 2), (1, 3), (0, 5), (1, 4), (1, 5)]
UNIT_OF = {unit: i for i, unit in enumerate(UNITS)}


def gelu(a):
    return a * (0.5 * (1.0 + jnp.tanh(0.7978845608028654 * (a + 0.044715 * (a * a * a)))))


def moe_kernel(nt, ne, x_hbm, dst_in, meta, wr, w0_hbm, w1_hbm, wo_hbm, out_ref, tok, dstb, w0, w1, wo, xbuf, part, hin, fin, ysum, back, acc, gate, outt,
               ld_sem, w_sem, xs_s, xs_r, dd_s, dd_r, ds_s, ds_r, ys_s, ys_r, bk_s, bk_r, fa_s, fa_r):
    n_tok, d = x_hbm.shape
    n_loc = w0_hbm.shape[0]
    n_exp = wr.shape[1]
    cap = 2 * CAP_FACTOR * n_tok // n_exp
    rows = n_loc * cap
    half, quart = n_tok // 2, n_tok // 4
    nx = ne // 2
    me, t = lax.axis_index("ep"), lax.axis_index("tp")
    cx, c = me // 2, me % 2
    xr, xl, xo = (cx + 1) % nx, (cx + nx - 1) % nx, (cx + 2) % nx
    sib = me + 1 - 2 * c
    tr, tl, to = (t + 1) % nt, (t + nt - 1) % nt, (t + 2) % nt
    has_b = c == t // 2

    def rcopy(src, dst, s, r, e=None, y=None):
        dev = {"ep": me if e is None else e, "tp": t if y is None else y}
        return pltpu.make_async_remote_copy(src_ref=src, dst_ref=dst, send_sem=s, recv_sem=r, device_id=dev, device_id_type=MESH)

    barrier = pltpu.get_barrier_semaphore()
    for k in range(1, ne):
        pl.semaphore_signal(barrier, inc=1, device_id={"ep": (me + k) % ne, "tp": t}, device_id_type=MESH)
    for y in (tr, tl):
        pl.semaphore_signal(barrier, inc=1, device_id={"ep": me, "tp": y}, device_id_type=MESH)
    xload = pltpu.make_async_copy(x_hbm, tok.at[me], ld_sem)
    xload.start()
    wloads = []
    for e in range(n_loc):
        for i, (h, v) in enumerate(((w0_hbm, w0), (w1_hbm, w1), (wo_hbm, wo))):
            wloads.append(pltpu.make_async_copy(h.at[e], v.at[e], w_sem.at[i, e]))
            wloads[-1].start()
    dstb[me] = dst_in[...]
    pl.semaphore_wait(barrier, ne - 1 + 2)
    xload.wait()

    sends = []

    def go(copy):
        copy.start()
        sends.append(copy)

    def own_half(h):
        return tok.at[me, pl.ds(half * h, half)]

    hc = pl.multiple_of(half * c, half)
    hs = pl.multiple_of(half * (1 - c), half)
    go(rcopy(tok.at[me, pl.ds(hs, half)], tok.at[me, pl.ds(hs, half)], dd_s.at[0], dd_r.at[0], e=sib))
    for k in range(1, ne):
        go(rcopy(dst_in, dstb.at[me], ds_s.at[k], ds_r.at[me], e=(me + k) % ne))

    def piece(j, off=0, n=half):
        return tok.at[j, pl.ds(pl.multiple_of(hc + off, quart), n)]

    ev, od = 2 * cx, 2 * cx + 1
    x_r0 = rcopy(piece(ev), piece(ev), xs_s.at[0], xs_r.at[0], e=2 * xr + c)
    x_r1 = rcopy(piece(od), piece(od), xs_s.at[1], xs_r.at[1], e=2 * xr + c)
    x_l0 = rcopy(piece(od), piece(od), xs_s.at[2], xs_r.at[2], e=2 * xl + c)
    x_l1 = rcopy(piece(ev), piece(ev), xs_s.at[3], xs_r.at[3], e=2 * xl + c)
    sends.extend((x_r0, x_r1, x_l0, x_l1))
    in_sib0 = rcopy(piece(sib), piece(sib), dd_s.at[0], dd_r.at[0])

    @pl.when(c == 0)
    def _():
        x_r0.start()
        in_sib0.wait_recv()
        x_l0.start()

    @pl.when(c == 1)
    def _():
        x_l0.start()
        in_sib0.wait_recv()
        x_r0.start()

    x_r1.start()
    x_l1.start()
    go(rcopy(piece(me), piece(me), dd_s.at[1], dd_r.at[1], e=sib))
    sib_rest = tok.at[sib, pl.ds(hs, half)]
    rcopy(sib_rest, sib_rest, dd_s.at[1], dd_r.at[1]).wait_recv()
    for k in range(1, ne):
        src = (me + k) % ne
        rcopy(dst_in, dstb.at[src], ds_s.at[k], ds_r.at[src]).wait_recv()

    phases = ((2 * cx, 2 * cx + 1), (2 * xl, 2 * xr + 1), (2 * xr, 2 * xl + 1), (2 * xo, 2 * xo + 1))

    def compute(p):
        slot = p % 2
        rb = min(256, rows)
        for s, j in enumerate(phases[p]):
            def gather(i, carry, s=s, j=j):
                want = lax.broadcasted_iota(jnp.int32, (rb, n_tok), 0) + (i * rb + rows * me)
                hit = (dstb[j, 0:1, :] == want) | (dstb[j, 1:2, :] == want)
                pick = jnp.where(hit, 1.0, 0.0).astype(BF16)
                got = jnp.dot(pick, tok[j], preferred_element_type=F32).astype(BF16)
                for q in range(rb // cap):
                    xbuf[i * (rb // cap) + q, s * cap:(s + 1) * cap, :] = got[q * cap:(q + 1) * cap]
                return carry
            lax.fori_loop(0, rows // rb, gather, 0)

        def ffn(e, carry):
            if p == 0:
                for i, (h, v) in enumerate(((w0_hbm, w0), (w1_hbm, w1), (wo_hbm, wo))):
                    pltpu.make_async_copy(h.at[e], v.at[e], w_sem.at[i, e]).wait()
            xe = xbuf[e]
            a = jnp.dot(xe, w0[e], preferred_element_type=F32)
            b = jnp.dot(xe, w1[e], preferred_element_type=F32)
            hid = (gelu(a) * b).astype(BF16)
            y = jnp.dot(hid, wo[e], preferred_element_type=F32).astype(BF16)
            for s in range(2):
                for k in range(d // LANES):
                    at = pl.multiple_of(UNIT_OF[s, k] * rows + e * cap, cap)
                    part[slot, pl.ds(at, cap), :] = y[s * cap:(s + 1) * cap, k * LANES:(k + 1) * LANES]
            return carry
        lax.fori_loop(0, n_loc, ffn, 0)

    blk = 3 * rows
    hb = blk // 2

    def block(p, y, h=None):
        lo, n = (0, blk) if h is None else (h * hb, hb)
        return part.at[p % 2, pl.ds(pl.multiple_of(y * blk + lo, hb), n)]

    ysends = {}

    def ysend(p, i, src, dst, y):
        copy = rcopy(src, dst, ys_s.at[p, i], ys_r.at[p, i], y=y)
        copy.start()
        ysends.setdefault(p, []).append(copy)

    def yrecv(p, i, dst):
        rcopy(dst, dst, ys_s.at[p, i], ys_r.at[p, i]).wait_recv()

    def rs_start(p):
        ysend(p, 0, block(p, to, 0), hin.at[p, 0], tr)
        ysend(p, 1, block(p, to, 1), hin.at[p, 1], tl)
        ysend(p, 2, block(p, tr, 1), fin.at[p, 0, pl.ds(hb, hb)], tr)
        ysend(p, 3, block(p, tl, 0), fin.at[p, 1, pl.ds(0, hb)], tl)

    def rs_mid(p):
        for i, y, h in ((0, tr, 0), (1, tl, 1)):
            yrecv(p, i, hin.at[p, i])
            ref = block(p, y, h)
            ref[...] = (ref[...].astype(F32) + hin[p, i].astype(F32)).astype(BF16)
            ysend(p, 4 + i, ref, fin.at[p, i, pl.ds(h * hb, hb)], y)

    def rs_final(p):
        yrecv(p, 2, fin.at[p, 0, pl.ds(hb, hb)])
        yrecv(p, 3, fin.at[p, 1, pl.ds(0, hb)])
        yrecv(p, 4, fin.at[p, 0, pl.ds(0, hb)])
        yrecv(p, 5, fin.at[p, 1, pl.ds(hb, hb)])
        total = block(p, t)[...].astype(F32) + fin[p, 0].astype(F32) + fin[p, 1].astype(F32)
        ysum[p] = total.astype(BF16)
        for copy in ysends.pop(p):
            copy.wait_send()

    col_a, col_b = pl.ds(0, LANES), pl.ds(LANES, LANES)

    def unit(p, u):
        return ysum.at[p, pl.ds(pl.multiple_of(u * rows, rows), rows)]

    waits = []

    def send_back(p):
        if p == 0:
            back[me, :, 0:LANES] = unit(p, 2 * c)[...]
            go(rcopy(unit(p, 2 - 2 * c), back.at[me, :, col_a], bk_s.at[p, 0], bk_r.at[me, 0], e=sib))
            other = rcopy(unit(p, 1), back.at[me, :, col_b], bk_s.at[p, 1], bk_r.at[me, 1], e=sib)

            @pl.when(has_b)
            def _():
                back[me, :, LANES:2 * LANES] = unit(p, 1)[...]

            @pl.when(jnp.logical_not(has_b))
            def _():
                other.start()
            waits.append((jnp.logical_not(has_b), other))
        else:
            je, jo = phases[p]
            go(rcopy(unit(p, 0), back.at[me, :, col_a], bk_s.at[p, 0], bk_r.at[me, 0], e=je))
            go(rcopy(unit(p, 2), back.at[me, :, col_a], bk_s.at[p, 2], bk_r.at[me, 0], e=jo))
            jb = je + (t // 2) * (jo - je)
            go(rcopy(unit(p, 1), back.at[me, :, col_b], bk_s.at[p, 1], bk_r.at[me, 1], e=jb))

    back_chip = (cx, xr + c * (xl - xr), xl + c * (xr - xl), xo)

    def combine(p):
        srcs = (me, sib) if p == 0 else (2 * back_chip[p], 2 * back_chip[p] + 1)
        for m in srcs[1:] if p == 0 else srcs:
            rcopy(back.at[m, :, col_a], back.at[m, :, col_a], bk_s.at[p, 0], bk_r.at[m, 0]).wait_recv()

            @pl.when(has_b)
            def _(m=m):
                rcopy(back.at[m, :, col_b], back.at[m, :, col_b], bk_s.at[p, 1], bk_r.at[m, 1]).wait_recv()

        rb = min(256, n_tok)

        def some(i, carry):
            r = pl.ds(pl.multiple_of(i * rb, rb), rb)
            lane = lax.broadcasted_iota(jnp.int32, (rb, rows), 1)
            sums = None
            for m in srcs:
                for q in range(2):
                    pick = jnp.where(lane == meta[r, 2 + q:3 + q] - rows * m, 1.0, 0.0).astype(BF16)
                    term = gate[r, q:q + 1] * jnp.dot(pick, back[m], preferred_element_type=F32)
                    sums = term if sums is None else sums + term
            acc[r, :] = sums if p == 0 else acc[r, :] + sums
            return carry
        lax.fori_loop(0, n_tok // rb, some, 0)

    def gates():
        w = wr[...]
        hi = w.astype(BF16)
        r1 = w - hi.astype(F32)
        mid = r1.astype(BF16)
        lo = (r1 - mid.astype(F32)).astype(BF16)
        rb = min(256, n_tok)

        def some(i, carry):
            r = pl.ds(pl.multiple_of(i * rb, rb), rb)
            xs = tok[me, r, :]
            logits = jnp.dot(xs, lo, preferred_element_type=F32) + jnp.dot(xs, mid, preferred_element_type=F32) + jnp.dot(xs, hi, preferred_element_type=F32)
            un = jnp.exp(logits - jnp.max(logits, axis=1, keepdims=True))
            prob = un / jnp.sum(un, axis=1, keepdims=True)
            lane = lax.broadcasted_iota(jnp.int32, (rb, n_exp), 1)
            p1 = jnp.sum(jnp.where(lane == meta[r, 0:1], prob, 0.0), axis=1, keepdims=True)
            p2 = jnp.sum(jnp.where(lane == meta[r, 1:2], prob, 0.0), axis=1, keepdims=True)
            both = p1 + p2
            gate[r, 0:1] = p1 / both
            gate[r, 1:2] = p2 / both
            return carry
        lax.fori_loop(0, n_tok // rb, some, 0)

    def xrecv(i, ref):
        rcopy(ref, ref, xs_s.at[i], xs_r.at[i]).wait_recv()

    def dsend(i, ref):
        go(rcopy(ref, ref, dd_s.at[i], dd_r.at[i], e=sib))

    def drecv(i, ref):
        rcopy(ref, ref, dd_s.at[i], dd_r.at[i]).wait_recv()

    def arrive(p):
        je, jo = phases[p]
        from_l, from_r = (je, jo) if p == 1 else (jo, je)
        i = p - 1
        xrecv(i, piece(from_l))
        go(rcopy(piece(from_l, 0, quart), piece(from_l, 0, quart), xs_s.at[4 + i], xs_r.at[4 + i], e=2 * xr + c))
        dsend(2 + 2 * i, piece(from_l))
        xrecv(2 + i, piece(from_r))
        go(rcopy(piece(from_r, quart, quart), piece(from_r, quart, quart), xs_s.at[6 + i], xs_r.at[6 + i], e=2 * xl + c))
        dsend(3 + 2 * i, piece(from_r))

    def spiece(j, off=0, n=half):
        return tok.at[j, pl.ds(pl.multiple_of(hs + off, quart), n)]

    def arrived(p):
        je, jo = phases[p]
        from_l, from_r = (je, jo) if p == 1 else (jo, je)
        i = p - 1
        drecv(2 + 2 * i, spiece(from_l))
        drecv(3 + 2 * i, spiece(from_r))

    far = (((4, 2 * xo, 0), (6, 2 * xo + 1, quart)), ((5, 2 * xo + 1, 0), (7, 2 * xo, quart)))

    def arrive_far():
        n = 6
        for group in far:
            for i, j, off in group:
                xrecv(i, piece(j, off, quart))
                dsend(n, piece(j, off, quart))
                n += 1

    def arrived_far():
        n = 6
        for group in far:
            for i, j, off in group:
                drecv(n, spiece(j, off, quart))
                n += 1

    compute(0)
    rs_start(0)
    gates()
    arrive(1)
    rs_mid(0)
    arrived(1)
    compute(1)
    rs_final(0)
    send_back(0)
    rs_start(1)
    arrive(2)
    rs_mid(1)
    arrived(2)
    compute(2)
    rs_final(1)
    send_back(1)
    rs_start(2)
    combine(0)
    arrive_far()
    rs_mid(2)
    arrived_far()
    compute(3)
    rs_final(2)
    send_back(2)
    rs_start(3)
    combine(1)
    rs_mid(3)
    combine(2)
    rs_final(3)
    send_back(3)
    combine(3)

    def own_col(y):
        return 2 * y - jnp.where(c == 0, y // (nt - 1), (y + nt - 1) // nt), jnp.where(c == 0, 2 * y + 1, 2 * y - 2)

    def owns_b(y):
        return c == y // 2

    ka, kb = own_col(t)
    outt[ka] = acc[:, 0:LANES].astype(BF16)

    @pl.when(has_b)
    def _():
        outt[kb] = acc[:, LANES:2 * LANES].astype(BF16)

    def hrow(k, h):
        return outt.at[k, pl.ds(h * half, half)]

    def fin_send(i, k, h, y, cond=None):
        copy = rcopy(hrow(k, h), hrow(k, h), fa_s.at[i], fa_r.at[i], y=y)
        if cond is None:
            copy.start()
            sends.append(copy)
        else:
            pl.when(cond)(copy.start)
            waits.append((cond, copy))

    def fin_recv(i, k, h, cond=None):
        copy = rcopy(hrow(k, h), hrow(k, h), fa_s.at[i], fa_r.at[i])
        if cond is None:
            copy.wait_recv()
        else:
            pl.when(cond)(copy.wait_recv)

    for h in range(2):
        fin_send(0 + h, ka, h, tr)
        fin_send(2 + h, ka, 1 - h, tl)
        fin_send(4 + h, kb, h, tr, has_b)
        fin_send(6 + h, kb, 1 - h, tl, has_b)
    (kal, kbl), (kar, kbr), (kao, kbo) = own_col(tl), own_col(tr), own_col(to)
    fin_recv(0, kal, 0)
    fin_send(8, kal, 0, tr)
    fin_recv(2, kar, 1)
    fin_send(9, kar, 1, tl)
    fin_recv(4, jnp.clip(kbl, 0, 5), 0, owns_b(tl))
    fin_send(10, jnp.clip(kbl, 0, 5), 0, tr, owns_b(tl))
    fin_recv(6, jnp.clip(kbr, 0, 5), 1, owns_b(tr))
    fin_send(11, jnp.clip(kbr, 0, 5), 1, tl, owns_b(tr))
    fin_recv(1, kal, 1)
    fin_recv(3, kar, 0)
    fin_recv(5, jnp.clip(kbl, 0, 5), 1, owns_b(tl))
    fin_recv(7, jnp.clip(kbr, 0, 5), 0, owns_b(tr))
    fin_recv(8, kao, 0)
    fin_recv(9, kao, 1)
    fin_recv(10, jnp.clip(kbo, 0, 5), 0, owns_b(to))
    fin_recv(11, jnp.clip(kbo, 0, 5), 1, owns_b(to))
    for k in range(d // LANES):
        out_ref[:, k * LANES:(k + 1) * LANES] = outt[k]
    for copy in sends:
        copy.wait_send()
    for cond, copy in waits:
        pl.when(cond)(copy.wait_send)


def solution(mesh):
    tok_spec = P(("dp", "ep"), None)
    w_in_spec = P("ep", None, "tp")
    w_out_spec = P("ep", "tp", None)
    nt, ne = mesh.shape["tp"], mesh.shape["ep"]

    def local_step(x_tok, w_router, w_gelu, w_lin, w_out, expert_idx, slot_idx):
        n_tok, d = x_tok.shape
        n_exp = w_router.shape[1]
        n_loc, _, f = w_gelu.shape
        cap = 2 * CAP_FACTOR * n_tok // n_exp
        rows = n_loc * cap
        me = lax.axis_index("ep")
        dest = jnp.where(slot_idx >= 0, expert_idx * cap + slot_idx - me * cap, -1)
        meta = jnp.concatenate([expert_idx, dest], axis=1)
        vmem = pl.BlockSpec(memory_space=pltpu.VMEM)
        hbm = pl.BlockSpec(memory_space=pl.ANY)
        dma = pltpu.SemaphoreType.DMA
        return pl.pallas_call(
            functools.partial(moe_kernel, nt, ne),
            out_shape=jax.ShapeDtypeStruct((n_tok, d), BF16),
            in_specs=[hbm, vmem, vmem, vmem, hbm, hbm, hbm],
            out_specs=vmem,
            scratch_shapes=[
                pltpu.VMEM((ne, n_tok, d), BF16),
                pltpu.VMEM((ne, 2, n_tok), jnp.int32),
                pltpu.VMEM((n_loc, d, f), BF16),
                pltpu.VMEM((n_loc, d, f), BF16),
                pltpu.VMEM((n_loc, f, d), BF16),
                pltpu.VMEM((n_loc, 2 * cap, d), BF16),
                pltpu.VMEM((2, 12 * rows, LANES), BF16),
                pltpu.VMEM((4, 2, 3 * rows // 2, LANES), BF16),
                pltpu.VMEM((4, 2, 3 * rows, LANES), BF16),
                pltpu.VMEM((4, 3 * rows, LANES), BF16),
                pltpu.VMEM((ne, rows, 2 * LANES), BF16),
                pltpu.VMEM((n_tok, 2 * LANES), F32),
                pltpu.VMEM((n_tok, 2), F32),
                pltpu.VMEM((d // LANES, n_tok, LANES), BF16),
                dma, dma((3, n_loc)), dma((8,)), dma((8,)), dma((10,)), dma((10,)), dma((ne,)), dma((ne,)),
                dma((4, 6)), dma((4, 6)), dma((4, 3)), dma((ne, 2)), dma((12,)), dma((12,)),
            ],
            compiler_params=pltpu.CompilerParams(collective_id=0, has_side_effects=True, vmem_limit_bytes=67043328),
            name="moe",
        )(x_tok, dest.T, meta, w_router, w_gelu, w_lin, w_out)

    return jax.shard_map(local_step, mesh=mesh, in_specs=(tok_spec, P(), w_in_spec, w_in_spec, w_out_spec, tok_spec, tok_spec), out_specs=tok_spec, check_vma=False)
```

```python
import functools

import jax
import jax.numpy as jnp
from jax import lax
from jax.experimental import pallas as pl
from jax.experimental.pallas import tpu as pltpu
from jax.sharding import PartitionSpec as P

CAP_FACTOR = 2
LANES = 128
SHARED = (256, 0)
MESH = pl.DeviceIdType.MESH
F32 = jnp.float32
BF16 = jnp.bfloat16
UNITS = [(0, 0), (0, 1), (1, 0), (0, 2), (0, 3), (1, 1), (0, 4), (1, 2), (1, 3), (0, 5), (1, 4), (1, 5)]
UNIT_OF = {unit: i for i, unit in enumerate(UNITS)}


def gelu(a):
    return a * (0.5 * (1.0 + jnp.tanh(0.7978845608028654 * (a + 0.044715 * (a * a * a)))))


def moe_kernel(nt, ne, x_hbm, wr_hbm, w0_hbm, w1_hbm, wo_hbm, exp_hbm, slot_hbm, out_ref, route, meta, wr, tok, dstb, w0, w1, wo, xbuf, part, hin, fin, ysum, back, acc, gate, outt,
               ld_sem, w_sem, xs_s, xs_r, xa_s, xa_r, ya_s, ya_r, dd_s, dd_r, ds_s, ds_r, ys_s, ys_r, bk_s, bk_r, fa_s, fa_r, st_sem):
    n_tok, d = x_hbm.shape
    n_loc = w0_hbm.shape[0]
    n_exp = wr.shape[0]
    cap = 2 * CAP_FACTOR * n_tok // n_exp
    rows = n_loc * cap
    half, quart = n_tok // 2, n_tok // 4
    nx = ne // 2
    me, t = lax.axis_index("ep"), lax.axis_index("tp")
    cx, c = me // 2, me % 2
    xr, xl, xo = (cx + 1) % nx, (cx + nx - 1) % nx, (cx + 2) % nx
    sib = me + 1 - 2 * c
    tr, tl, to = (t + 1) % nt, (t + nt - 1) % nt, (t + 2) % nt
    has_b = c == t // 2

    def rcopy(src, dst, s, r, e=None, y=None):
        dev = {"ep": me if e is None else e, "tp": t if y is None else y}
        return pltpu.make_async_remote_copy(src_ref=src, dst_ref=dst, send_sem=s, recv_sem=r, device_id=dev, device_id_type=MESH)

    barrier = pltpu.get_barrier_semaphore()
    for k in range(1, ne):
        pl.semaphore_signal(barrier, inc=1, device_id={"ep": (me + k) % ne, "tp": t}, device_id_type=MESH)
    for y in (tr, tl):
        pl.semaphore_signal(barrier, inc=1, device_id={"ep": me, "tp": y}, device_id_type=MESH)
    xload = pltpu.make_async_copy(x_hbm, tok.at[me], ld_sem.at[0])
    eload = pltpu.make_async_copy(exp_hbm, route.at[0], ld_sem.at[1])
    sload = pltpu.make_async_copy(slot_hbm, route.at[1], ld_sem.at[2])
    rload = pltpu.make_async_copy(wr_hbm, wr, ld_sem.at[3])
    eload.start()
    sload.start()
    xload.start()
    eload.wait()
    sload.wait()
    slots = route[1]
    dest = jnp.where(slots >= 0, route[0] * cap + slots - me * cap, -1)
    dstb[me] = dest
    with jax.named_scope("barrier"):
        pl.semaphore_wait(barrier, ne - 1 + 2)
    with jax.named_scope("xload"):
        xload.wait()

    sends = []

    def go(copy):
        copy.start()
        sends.append(copy)

    def own_half(h):
        return tok.at[me, pl.ds(half * h, half)]

    hc = pl.multiple_of(half * c, half)
    hs = pl.multiple_of(half * (1 - c), half)
    go(rcopy(tok.at[me, pl.ds(hs, half)], tok.at[me, pl.ds(hs, half)], dd_s.at[0], dd_r.at[0], e=sib))
    for k in range(1, ne):
        go(rcopy(dstb.at[me], dstb.at[me], ds_s.at[k], ds_r.at[me], e=(me + k) % ne))

    def piece(j, off=0, n=half):
        return tok.at[j, pl.ds(pl.multiple_of(hc + off, quart), n)]

    def alone(j, i):
        return tok.at[j, pl.ds(hc, half - SHARED[i])]

    def share(j, i, y, h=None):
        n = SHARED[i] // nt
        lo, m = (0, n) if h is None else (h * n // 2, n // 2)
        return tok.at[j, pl.ds(pl.multiple_of(hc + half - SHARED[i] + y * n + lo, 16), m)]

    ev, od = 2 * cx, 2 * cx + 1

    outgoing = []
    for n, (j, x) in enumerate(((ev, xr), (od, xr), (od, xl), (ev, xl))):
        i = n % 2
        outgoing.append([])
        if SHARED[i]:
            outgoing[n].append(rcopy(share(j, i, t), share(j, i, t), xa_s.at[n], xa_r.at[n], e=2 * x + c))
        if SHARED[i] < half:
            outgoing[n].append(rcopy(alone(j, i), alone(j, i), xs_s.at[n], xs_r.at[n], e=2 * x + c))
        sends.extend(outgoing[n])

    def xsend(n):
        for copy in outgoing[n]:
            copy.start()

    in_sib0 = rcopy(piece(sib), piece(sib), dd_s.at[0], dd_r.at[0])

    @pl.when(c == 0)
    def _():
        xsend(0)
        in_sib0.wait_recv()
        xsend(2)
        xsend(1)
        xsend(3)

    @pl.when(c == 1)
    def _():
        xsend(2)
        in_sib0.wait_recv()
        xsend(0)
        xsend(3)
        xsend(1)

    go(rcopy(piece(me), piece(me), dd_s.at[1], dd_r.at[1], e=sib))
    for e in range(n_loc):
        for i, (h, v) in enumerate(((w0_hbm, w0), (w1_hbm, w1), (wo_hbm, wo))):
            pltpu.make_async_copy(h.at[e], v.at[e], w_sem.at[i, e]).start()
    rload.start()
    meta[...] = jnp.concatenate([route[0], dest, jnp.zeros((4, n_tok), jnp.int32)], axis=0).T
    sib_rest = tok.at[sib, pl.ds(hs, half)]
    with jax.named_scope("sibrest"):
        rcopy(sib_rest, sib_rest, dd_s.at[1], dd_r.at[1]).wait_recv()

    def dst_wait(src):
        rcopy(dstb.at[src], dstb.at[src], ds_s.at[1], ds_r.at[src]).wait_recv()

    phases = ((2 * cx, 2 * cx + 1), (2 * xl, 2 * xr + 1), (2 * xr, 2 * xl + 1), (2 * xo, 2 * xo + 1))

    nq = 2
    eq = n_loc // nq
    rq = rows // nq

    def gather_rows(p):
        rb = min(256, rows)
        for s, j in enumerate(phases[p]):
            if p > 0:
                dst_wait(j)
            elif s == 0:
                dst_wait(sib)

            def gather(i, carry, s=s, j=j):
                want = lax.broadcasted_iota(jnp.int32, (rb, n_tok), 0) + (i * rb + rows * me)
                hit = (dstb[j, 0:1, :] == want) | (dstb[j, 1:2, :] == want)
                pick = jnp.where(hit, 1.0, 0.0).astype(BF16)
                got = jnp.dot(pick, tok[j], preferred_element_type=F32).astype(BF16)
                for q in range(rb // cap):
                    xbuf[i * (rb // cap) + q, s * cap:(s + 1) * cap, :] = got[q * cap:(q + 1) * cap]
                return carry
            lax.fori_loop(0, rows // rb, gather, 0)

    def experts(p, q):
        slot = p % 2

        def ffn(e, carry):
            if p == 0:
                for i, (h, v) in enumerate(((w0_hbm, w0), (w1_hbm, w1), (wo_hbm, wo))):
                    pltpu.make_async_copy(h.at[e], v.at[e], w_sem.at[i, e]).wait()
            xe = xbuf[e]
            a = jnp.dot(xe, w0[e], preferred_element_type=F32)
            b = jnp.dot(xe, w1[e], preferred_element_type=F32)
            hid = (gelu(a) * b).astype(BF16)
            y = jnp.dot(hid, wo[e], preferred_element_type=F32).astype(BF16)
            for s in range(2):
                for k in range(d // LANES):
                    at = pl.multiple_of(UNIT_OF[s, k] * rq + (e - q * eq) * cap, cap)
                    part[slot, q, pl.ds(at, cap), :] = y[s * cap:(s + 1) * cap, k * LANES:(k + 1) * LANES]
            return carry
        lax.fori_loop(q * eq, (q + 1) * eq, ffn, 0)

    blk = 3 * rq
    hb = blk // 2

    def block(p, q, y, h=None):
        lo, n = (0, blk) if h is None else (h * hb, hb)
        return part.at[p % 2, q, pl.ds(pl.multiple_of(y * blk + lo, hb), n)]

    ysends = {}

    def ysend(p, q, i, src, dst, y):
        copy = rcopy(src, dst, ys_s.at[p, q, i], ys_r.at[p, q, i], y=y)
        copy.start()
        ysends.setdefault((p, q), []).append(copy)

    def yrecv(p, q, i, dst):
        rcopy(dst, dst, ys_s.at[p, q, i], ys_r.at[p, q, i]).wait_recv()

    def rs_start(p, q):
        ysend(p, q, 0, block(p, q, to, 0), hin.at[p, q, 0], tr)
        ysend(p, q, 1, block(p, q, to, 1), hin.at[p, q, 1], tl)
        ysend(p, q, 2, block(p, q, tr, 1), fin.at[p, q, 0, pl.ds(hb, hb)], tr)
        ysend(p, q, 3, block(p, q, tl, 0), fin.at[p, q, 1, pl.ds(0, hb)], tl)

    def rs_mid(p, q):
        for i, y, h in ((0, tr, 0), (1, tl, 1)):
            yrecv(p, q, i, hin.at[p, q, i])
            ref = block(p, q, y, h)
            ref[...] = (ref[...].astype(F32) + hin[p, q, i].astype(F32)).astype(BF16)
            ysend(p, q, 4 + i, ref, fin.at[p, q, i, pl.ds(h * hb, hb)], y)

    def rs_final(p, q):
        yrecv(p, q, 2, fin.at[p, q, 0, pl.ds(hb, hb)])
        yrecv(p, q, 3, fin.at[p, q, 1, pl.ds(0, hb)])
        yrecv(p, q, 4, fin.at[p, q, 0, pl.ds(0, hb)])
        yrecv(p, q, 5, fin.at[p, q, 1, pl.ds(hb, hb)])
        total = block(p, q, t)[...].astype(F32) + fin[p, q, 0].astype(F32) + fin[p, q, 1].astype(F32)
        ysum[p, q] = total.astype(BF16)
        for copy in ysends.pop((p, q)):
            copy.wait_send()
        send_back(p, q)

    col_a, col_b = pl.ds(0, LANES), pl.ds(LANES, LANES)

    def unit(p, q, u):
        return ysum.at[p, q, pl.ds(pl.multiple_of(u * rq, rq), rq)]

    waits = []

    def home(m, q, col):
        return back.at[m, pl.ds(q * rq, rq), col]

    def send_back(p, q):
        if p == 0:
            back[me, q * rq:(q + 1) * rq, 0:LANES] = unit(p, q, 2 * c)[...]
            go(rcopy(unit(p, q, 2 - 2 * c), home(me, q, col_a), bk_s.at[p, q, 0], bk_r.at[me, q, 0], e=sib))
            other = rcopy(unit(p, q, 1), home(me, q, col_b), bk_s.at[p, q, 1], bk_r.at[me, q, 1], e=sib)

            @pl.when(has_b)
            def _():
                back[me, q * rq:(q + 1) * rq, LANES:2 * LANES] = unit(p, q, 1)[...]

            @pl.when(jnp.logical_not(has_b))
            def _():
                other.start()
            waits.append((jnp.logical_not(has_b), other))
        else:
            je, jo = phases[p]
            go(rcopy(unit(p, q, 0), home(me, q, col_a), bk_s.at[p, q, 0], bk_r.at[me, q, 0], e=je))
            go(rcopy(unit(p, q, 2), home(me, q, col_a), bk_s.at[p, q, 2], bk_r.at[me, q, 0], e=jo))
            jb = je + (t // 2) * (jo - je)
            go(rcopy(unit(p, q, 1), home(me, q, col_b), bk_s.at[p, q, 1], bk_r.at[me, q, 1], e=jb))

    back_chip = (cx, xr + c * (xl - xr), xl + c * (xr - xl), xo)

    def combine(p):
        srcs = (me, sib) if p == 0 else (2 * back_chip[p], 2 * back_chip[p] + 1)
        for m in srcs[1:] if p == 0 else srcs:
            for q in range(nq):
                rcopy(home(m, q, col_a), home(m, q, col_a), bk_s.at[p, q, 0], bk_r.at[m, q, 0]).wait_recv()

            @pl.when(has_b)
            def _(m=m):
                for q in range(nq):
                    rcopy(home(m, q, col_b), home(m, q, col_b), bk_s.at[p, q, 1], bk_r.at[m, q, 1]).wait_recv()

        def some(i, carry):
            r = pl.ds(pl.multiple_of(i * quart, quart), quart)
            lane = lax.broadcasted_iota(jnp.int32, (quart, rows), 1)
            sums = None
            for m in srcs:
                for q in range(2):
                    pick = jnp.where(lane == meta[r, 2 + q:3 + q] - rows * m, 1.0, 0.0).astype(BF16)
                    term = gate[r, q:q + 1] * jnp.dot(pick, back[m], preferred_element_type=F32)
                    sums = term if sums is None else sums + term
            if p < 3:
                acc[r, :] = sums if p == 0 else acc[r, :] + sums
            else:
                full = (acc[r, :] + sums).astype(BF16)
                outt[ka, r, :] = full[:, :LANES]

                @pl.when(has_b)
                def _():
                    outt[kb, r, :] = full[:, LANES:]
                spread(i)
            return carry
        if p < 3:
            lax.fori_loop(0, n_tok // quart, some, 0)
        else:
            for i in range(n_tok // quart):
                some(i, 0)

    def own_col(y):
        return 2 * y - jnp.where(c == 0, y // (nt - 1), (y + nt - 1) // nt), jnp.clip(jnp.where(c == 0, 2 * y + 1, 2 * y - 2), 0, d // LANES - 1)

    def owns_b(y):
        return c == y // 2

    ka, kb = own_col(t)
    always = None

    def col_part(k, i):
        return outt.at[k, pl.ds(i * quart, quart)]

    def store(k, i, cond):
        pltpu_copy = pltpu.make_async_copy(col_part(k, i), out_ref.at[pl.ds(i * quart, quart), pl.ds(pl.multiple_of(k * LANES, LANES), LANES)], st_sem.at[k, i])
        do(cond, pltpu_copy.start)

    def do(cond, f):
        if cond is None:
            f()
        else:
            pl.when(cond)(f)

    def col_send(n, k, i, y, cond):
        copy = rcopy(col_part(k, i), col_part(k, i), fa_s.at[n, i], fa_r.at[n, i], y=y)
        do(cond, copy.start)
        waits.append((cond, copy))

    def col_recv(n, k, i, cond):
        copy = rcopy(col_part(k, i), col_part(k, i), fa_s.at[n, i], fa_r.at[n, i])
        do(cond, copy.wait_recv)
        store(k, i, cond)

    def spread(i):
        for n, k, cond in ((0, ka, None), (1, kb, has_b)):
            col_send(n, k, i, tr, cond)
            col_send(2 + n, k, i, tl, cond)
            store(k, i, cond)

    def collect():
        (kal, kbl), (kar, kbr), (kao, kbo) = own_col(tl), own_col(tr), own_col(to)
        for i in range(n_tok // quart):
            for n, k, cond in ((0, kal, None), (1, kbl, owns_b(tl))):
                col_recv(n, k, i, cond)
                if i % 2 == 0:
                    col_send(4 + n, k, i, tr, cond)
            for n, k, cond in ((2, kar, None), (3, kbr, owns_b(tr))):
                col_recv(n, k, i, cond)
                if i % 2 == 1:
                    col_send(2 + n, k, i, tl, cond)
        for i in range(n_tok // quart):
            for n, k, cond in ((4, kao, None), (5, kbo, owns_b(to))):
                col_recv(n, k, i, cond)

    def gates():
        rload.wait()
        w = wr[...]
        hi = w.astype(BF16)
        r1 = w - hi.astype(F32)
        mid = r1.astype(BF16)
        lo = (r1 - mid.astype(F32)).astype(BF16)
        rb = min(256, n_tok)

        def some(i, carry):
            r = pl.ds(pl.multiple_of(i * rb, rb), rb)
            xs = tok[me, r, :]
            logits = sum(lax.dot_general(xs, v, (((1,), (1,)), ((), ())), preferred_element_type=F32) for v in (lo, mid, hi))
            un = jnp.exp(logits - jnp.max(logits, axis=1, keepdims=True))
            prob = un / jnp.sum(un, axis=1, keepdims=True)
            lane = lax.broadcasted_iota(jnp.int32, (rb, n_exp), 1)
            p1 = jnp.sum(jnp.where(lane == meta[r, 0:1], prob, 0.0), axis=1, keepdims=True)
            p2 = jnp.sum(jnp.where(lane == meta[r, 1:2], prob, 0.0), axis=1, keepdims=True)
            both = p1 + p2
            gate[r, 0:1] = p1 / both
            gate[r, 1:2] = p2 / both
            return carry
        lax.fori_loop(0, n_tok // rb, some, 0)

    def xrecv(i, ref):
        rcopy(ref, ref, xs_s.at[i], xs_r.at[i]).wait_recv()

    def dsend(i, ref):
        go(rcopy(ref, ref, dd_s.at[i], dd_r.at[i], e=sib))

    def drecv(i, ref):
        rcopy(ref, ref, dd_s.at[i], dd_r.at[i]).wait_recv()

    def pieces(p):
        je, jo = phases[p]
        return (je, jo) if p == 1 else (jo, je)

    def share_out(p):
        i = p - 1
        for dr, j in enumerate(pieces(p)) if SHARED[i] else ():
            mine = share(j, i, t)
            rcopy(mine, mine, xa_s.at[2 * dr + i], xa_r.at[2 * dr + i]).wait_recv()
            go(rcopy(mine, mine, ya_s.at[i, dr, 0], ya_r.at[i, dr, 0], y=tr))
            go(rcopy(mine, mine, ya_s.at[i, dr, 1], ya_r.at[i, dr, 1], y=tl))

    def share_on(p):
        i = p - 1
        for dr, j in enumerate(pieces(p)) if SHARED[i] else ():
            for k, y, far_y in ((0, tl, tr), (1, tr, tl)):
                got = share(j, i, y)
                rcopy(got, got, ya_s.at[i, dr, k], ya_r.at[i, dr, k]).wait_recv()
                on = share(j, i, y, k)
                go(rcopy(on, on, ya_s.at[i, dr, 2 + k], ya_r.at[i, dr, 2 + k], y=far_y))

    def share_in(p):
        i = p - 1
        for dr, j in enumerate(pieces(p)) if SHARED[i] else ():
            for k in range(2):
                got = share(j, i, to, k)
                rcopy(got, got, ya_s.at[i, dr, 2 + k], ya_r.at[i, dr, 2 + k]).wait_recv()

    def arrive(p):
        from_l, from_r = pieces(p)
        i = p - 1
        share_in(p)
        if SHARED[i] < half:
            xrecv(i, alone(from_l, i))
        go(rcopy(piece(from_l, 0, quart), piece(from_l, 0, quart), xs_s.at[4 + i], xs_r.at[4 + i], e=2 * xr + c))
        dsend(2 + 2 * i, piece(from_l))
        if SHARED[i] < half:
            xrecv(2 + i, alone(from_r, i))
        go(rcopy(piece(from_r, quart, quart), piece(from_r, quart, quart), xs_s.at[6 + i], xs_r.at[6 + i], e=2 * xl + c))
        dsend(3 + 2 * i, piece(from_r))

    def spiece(j, off=0, n=half):
        return tok.at[j, pl.ds(pl.multiple_of(hs + off, quart), n)]

    def arrived(p):
        je, jo = phases[p]
        from_l, from_r = (je, jo) if p == 1 else (jo, je)
        i = p - 1
        drecv(2 + 2 * i, spiece(from_l))
        drecv(3 + 2 * i, spiece(from_r))

    far = (((4, 2 * xo, 0), (6, 2 * xo + 1, quart)), ((5, 2 * xo + 1, 0), (7, 2 * xo, quart)))

    def arrive_far():
        n = 6
        for group in far:
            for i, j, off in group:
                xrecv(i, piece(j, off, quart))
                dsend(n, piece(j, off, quart))
                n += 1

    def arrived_far():
        n = 6
        for group in far:
            for i, j, off in group:
                drecv(n, spiece(j, off, quart))
                n += 1

    plan = [
        (gather_rows, 0), (share_out, 1), (experts, 0, 0), (rs_start, 0, 0), (experts, 0, 1), (share_on, 1), (rs_start, 0, 1),
        (gates,), (rs_mid, 0, 0), (arrive, 1), (arrived, 1),
        (gather_rows, 1), (rs_mid, 0, 1), (experts, 1, 0), (rs_start, 1, 0), (rs_final, 0, 0), (experts, 1, 1), (rs_start, 1, 1), (rs_final, 0, 1),
        (arrive, 2), (rs_mid, 1, 0), (arrived, 2),
        (gather_rows, 2), (rs_mid, 1, 1), (experts, 2, 0), (rs_start, 2, 0), (rs_final, 1, 0), (experts, 2, 1), (rs_start, 2, 1), (rs_final, 1, 1),
        (combine, 0), (rs_mid, 2, 0), (rs_mid, 2, 1), (rs_final, 2, 0), (arrive_far,), (arrived_far,),
        (gather_rows, 3), (rs_final, 2, 1), (experts, 3, 0), (rs_start, 3, 0), (experts, 3, 1), (rs_start, 3, 1),
        (rs_mid, 3, 0), (combine, 1), (rs_mid, 3, 1), (combine, 2), (rs_final, 3, 0), (rs_final, 3, 1), (combine, 3), (collect,),
    ]
    for f, *at in plan:
        with jax.named_scope(f.__name__ + "".join(str(v) for v in at)):
            f(*at)

    for copy in sends:
        copy.wait_send()
    for cond, copy in waits:
        do(cond, copy.wait_send)
    for k in range(d // LANES):
        for i in range(n_tok // quart):
            pltpu.make_async_copy(col_part(k, i), out_ref.at[pl.ds(i * quart, quart), pl.ds(k * LANES, LANES)], st_sem.at[k, i]).wait()


def solution(mesh):
    tok_spec = P(("dp", "ep"), None)
    w_in_spec = P("ep", None, "tp")
    w_out_spec = P("ep", "tp", None)
    nt, ne = mesh.shape["tp"], mesh.shape["ep"]

    def local_step(x_tok, w_router, w_gelu, w_lin, w_out, expert_idx, slot_idx):
        n_tok, d = x_tok.shape
        n_exp = w_router.shape[1]
        n_loc, _, f = w_gelu.shape
        cap = 2 * CAP_FACTOR * n_tok // n_exp
        rows = n_loc * cap
        hbm = pl.BlockSpec(memory_space=pl.ANY)
        dma = pltpu.SemaphoreType.DMA
        return pl.pallas_call(
            functools.partial(moe_kernel, nt, ne),
            out_shape=jax.ShapeDtypeStruct((n_tok, d), BF16),
            in_specs=[hbm] * 7,
            out_specs=hbm,
            scratch_shapes=[
                pltpu.VMEM((2, 2, n_tok), jnp.int32),
                pltpu.VMEM((n_tok, 8), jnp.int32),
                pltpu.VMEM((n_exp, d), F32),
                pltpu.VMEM((ne, n_tok, d), BF16),
                pltpu.VMEM((ne, 2, n_tok), jnp.int32),
                pltpu.VMEM((n_loc, d, f), BF16),
                pltpu.VMEM((n_loc, d, f), BF16),
                pltpu.VMEM((n_loc, f, d), BF16),
                pltpu.VMEM((n_loc, 2 * cap, d), BF16),
                pltpu.VMEM((2, 2, 6 * rows, LANES), BF16),
                pltpu.VMEM((4, 2, 2, 3 * rows // 4, LANES), BF16),
                pltpu.VMEM((4, 2, 2, 3 * rows // 2, LANES), BF16),
                pltpu.VMEM((4, 2, 3 * rows // 2, LANES), BF16),
                pltpu.VMEM((ne, rows, 2 * LANES), BF16),
                pltpu.VMEM((n_tok, 2 * LANES), F32),
                pltpu.VMEM((n_tok, 2), F32),
                pltpu.VMEM((d // LANES, n_tok, LANES), BF16),
                dma((4,)), dma((3, n_loc)), dma((8,)), dma((8,)), dma((4,)), dma((4,)), dma((2, 2, 4)), dma((2, 2, 4)), dma((10,)), dma((10,)), dma((ne,)), dma((ne,)),
                dma((4, 2, 6)), dma((4, 2, 6)), dma((4, 2, 3)), dma((ne, 2, 2)), dma((6, 4)), dma((6, 4)), dma((d // LANES, 4)),
            ],
            compiler_params=pltpu.CompilerParams(collective_id=0, has_side_effects=True, vmem_limit_bytes=67043328),
            name="moe",
        )(x_tok, w_router.T, w_gelu, w_lin, w_out, expert_idx.T, slot_idx.T)

    return jax.shard_map(local_step, mesh=mesh, in_specs=(tok_spec, P(), w_in_spec, w_in_spec, w_out_spec, tok_spec, tok_spec), out_specs=tok_spec, check_vma=False)
```

```python
import functools

import jax
import jax.numpy as jnp
from jax import lax
from jax.experimental import pallas as pl
from jax.experimental.pallas import tpu as pltpu
from jax.sharding import PartitionSpec as P

CAP_FACTOR = 2
LANES = 128
MESH = pl.DeviceIdType.MESH
F32 = jnp.float32
BF16 = jnp.bfloat16
UNITS = [(0, 0), (0, 1), (1, 0), (0, 2), (0, 3), (1, 1), (0, 4), (1, 2), (1, 3), (0, 5), (1, 4), (1, 5)]
UNIT_OF = {unit: i for i, unit in enumerate(UNITS)}
CHUNKS = ((4, 4), (4, 4), (4, 4), (3, 3, 2))


def gelu(a):
    return a * (0.5 * (1.0 + jnp.tanh(0.7978845608028654 * (a + 0.044715 * (a * a * a)))))


def moe_kernel(nt, ne, x_hbm, wr_hbm, w0_hbm, w1_hbm, wo_hbm, exp_hbm, slot_hbm, out_ref, route, meta, wr, tok, dstb, wts, xbuf, part, hin, fin, ysum, back, acc,
               gate, outt, ld_sem, w_sem, xs_s, xs_r, xa_r, ya_s, ya_r, dd_s, dd_r, ds_s, ds_r, ys_s, ys_r, bk_s, bk_r, fa_s, fa_r, st_sem):
    n_tok, d = x_hbm.shape
    n_loc = w0_hbm.shape[0]
    n_exp = wr.shape[0]
    cap = 2 * CAP_FACTOR * n_tok // n_exp
    rows = n_loc * cap
    half, quart = n_tok // 2, n_tok // 4
    n_col = d // LANES
    nx = ne // 2
    me, t = lax.axis_index("ep"), lax.axis_index("tp")
    cx, c = me // 2, me % 2
    xr, xl, xo = (cx + 1) % nx, (cx + nx - 1) % nx, (cx + 2) % nx
    sib = me + 1 - 2 * c
    tr, tl, to = (t + 1) % nt, (t + nt - 1) % nt, (t + 2) % nt
    has_b = c == t // 2

    def rcopy(src, dst, s, r, e=None, y=None):
        dev = {"ep": me if e is None else e, "tp": t if y is None else y}
        return pltpu.make_async_remote_copy(src_ref=src, dst_ref=dst, send_sem=s, recv_sem=r, device_id=dev, device_id_type=MESH)

    def received(ref, r):
        rcopy(ref, ref, ds_s, r).wait_recv()

    def sent(ref, s):
        rcopy(ref, ref, s, ds_r.at[0]).wait_send()

    def apart(f):
        pl.when(t >= 0)(f)

    barrier = pltpu.get_barrier_semaphore()
    for k in range(1, ne):
        pl.semaphore_signal(barrier, inc=1, device_id={"ep": (me + k) % ne, "tp": t}, device_id_type=MESH)
    for y in (tr, tl):
        pl.semaphore_signal(barrier, inc=1, device_id={"ep": me, "tp": y}, device_id_type=MESH)
    xload = pltpu.make_async_copy(x_hbm, tok.at[me], ld_sem.at[0])
    eload = pltpu.make_async_copy(exp_hbm, route.at[0], ld_sem.at[1])
    sload = pltpu.make_async_copy(slot_hbm, route.at[1], ld_sem.at[2])
    rload = pltpu.make_async_copy(wr_hbm, wr, ld_sem.at[3])
    eload.start()
    sload.start()
    xload.start()
    eload.wait()
    sload.wait()
    slots = route[1]
    dest = jnp.where(slots >= 0, route[0] * cap + slots - me * cap, -1)
    dstb[me] = dest
    with jax.named_scope("barrier"):
        pl.semaphore_wait(barrier, ne - 1 + 2)
    xload.wait()

    hc = pl.multiple_of(half * c, half)
    hs = pl.multiple_of(half * (1 - c), half)
    give = tok.at[me, pl.ds(hs, half)]
    rcopy(give, give, dd_s, dd_r.at[0], e=sib).start()
    for k in range(1, ne):
        e = (me + k) % ne
        rcopy(dstb.at[me], dstb.at[me], ds_s, ds_r.at[jnp.where(e == sib, 0, 1)], e=e).start()

    def piece(j, off=0, n=half):
        return tok.at[j, pl.ds(pl.multiple_of(hc + off, quart), n)]

    def spiece(j, off=0, n=half):
        return tok.at[j, pl.ds(pl.multiple_of(hs + off, quart), n)]

    def share(j, y, h=None):
        n = quart // nt
        lo, m = (0, n) if h is None else (h * n // 2, n // 2)
        return tok.at[j, pl.ds(pl.multiple_of(hc + quart + y * n + lo, 16), m)]

    ev, od = 2 * cx, 2 * cx + 1
    outgoing = []
    for n, (j, x) in enumerate(((ev, xr), (od, xr), (od, xl), (ev, xl))):
        first, sem = (share(j, t), xs_s.at[1]) if n % 2 == 0 else (piece(j, quart, quart), xs_s.at[2])
        outgoing.append([
            rcopy(first, first, sem, xa_r.at[n], e=2 * x + c),
            rcopy(piece(j, 0, quart), piece(j, 0, quart), xs_s.at[0], xs_r.at[n], e=2 * x + c),
        ])

    def xsend(n):
        for copy in outgoing[n]:
            copy.start()

    @pl.when(c == 0)
    def _():
        xsend(0)
        received(piece(sib), dd_r.at[0])
        xsend(2)
        xsend(1)
        xsend(3)

    @pl.when(c == 1)
    def _():
        xsend(2)
        received(piece(sib), dd_r.at[0])
        xsend(0)
        xsend(3)
        xsend(1)

    rcopy(piece(me), piece(me), dd_s, dd_r.at[1], e=sib).start()
    for e in range(n_loc):
        for i, h in enumerate((w0_hbm, w1_hbm, wo_hbm)):
            pltpu.make_async_copy(h.at[e], wts.at[e, i], w_sem.at[e]).start()
    rload.start()
    meta[...] = jnp.concatenate([route[0], dest, jnp.zeros((4, n_tok), jnp.int32)], axis=0).T

    phases = ((2 * cx, 2 * cx + 1), (2 * xl, 2 * xr + 1), (2 * xr, 2 * xl + 1), (2 * xo, 2 * xo + 1))

    def pieces(p):
        return phases[1] if p == 1 else phases[2][::-1]

    def span(p, q):
        e0 = sum(CHUNKS[p][:q])
        return e0, CHUNKS[p][q]

    def gather_shard(p, q, s, j):
        e0, n = span(p, q)

        def run():
            want = lax.broadcasted_iota(jnp.int32, (n * cap, n_tok), 0) + (e0 * cap + rows * me)
            hit = (dstb[j, 0:1, :] == want) | (dstb[j, 1:2, :] == want)
            pick = jnp.where(hit, 1.0, 0.0).astype(BF16)
            got = jnp.dot(pick, tok[j], preferred_element_type=F32).astype(BF16)
            for i in range(n):
                xbuf[e0 + i, pl.ds(pl.multiple_of(s * cap, cap), cap), :] = got[i * cap:(i + 1) * cap]
        apart(run)

    def gather_rows(p, q):
        if p == 0:
            gather_shard(p, q, c, me)
            if q == 0:
                received(spiece(sib), dd_r.at[1])
                received(dstb.at[0], ds_r.at[0])
            gather_shard(p, q, 1 - c, sib)
            return
        if p == 1 and q == 0:
            received(dstb.at[pl.ds(0, ne - 2)], ds_r.at[1])
        for s, j in enumerate(phases[p]):
            gather_shard(p, q, s, j)

    def experts(p, q):
        e0, n = span(p, q)
        base = 12 * cap * e0
        slot = p % 2

        def ffn(e):
            if p == 0:
                pltpu.make_async_copy(wts.at[e], wts.at[e], w_sem.at[e]).wait()
            xe = xbuf[e]
            a = jnp.dot(xe, wts[e, 0], preferred_element_type=F32)
            b = jnp.dot(xe, wts[e, 1], preferred_element_type=F32)
            hid = (gelu(a) * b).astype(BF16)
            y = jnp.dot(hid, wts[e, 2], preferred_element_type=F32).astype(BF16)
            for s in range(2):
                for k in range(n_col):
                    at = base + (UNIT_OF[s, k] * n + e - e0) * cap
                    part[slot, at:at + cap, :] = y[s * cap:(s + 1) * cap, k * LANES:(k + 1) * LANES]

        def run():
            for e in range(e0, e0 + n):
                ffn(e)
        apart(run)

    def block(p, q, y, h=None):
        e0, n = span(p, q)
        blk = 3 * n * cap
        lo, m = (0, blk) if h is None else (h * blk // 2, blk // 2)
        return part.at[p % 2, pl.ds(pl.multiple_of(12 * cap * e0 + y * blk + lo, blk // 2), m)]

    def hin_of(p, q, i):
        e0, n = span(p, q)
        return hin.at[p, i, pl.ds(3 * cap * e0 // 2, 3 * cap * n // 2)]

    def fin_of(p, q, i, h):
        e0, n = span(p, q)
        blk = 3 * n * cap
        return fin.at[p, i, pl.ds(3 * cap * e0 + h * blk // 2, blk // 2)]

    def rs_start(p, q):
        for i, src, dst, sem, y in (
            (0, block(p, q, to, 0), hin_of(p, q, 0), ys_r.at[p, q, 0], tr),
            (1, block(p, q, to, 1), hin_of(p, q, 1), ys_r.at[p, q, 1], tl),
            (2, block(p, q, tr, 1), fin_of(p, q, 0, 1), ys_r.at[p, q, 2], tr),
            (3, block(p, q, tl, 0), fin_of(p, q, 1, 0), ys_r.at[p, q, 2], tl),
        ):
            rcopy(src, dst, ys_s.at[p, q], sem, y=y).start()

    def rs_mid(p, q):
        for i, y, h in ((0, tr, 0), (1, tl, 1)):
            received(hin_of(p, q, i), ys_r.at[p, q, i])
            ref = block(p, q, y, h)
            ref[...] = (ref[...].astype(F32) + hin_of(p, q, i)[...].astype(F32)).astype(BF16)
            rcopy(ref, fin_of(p, q, i, h), ys_s.at[p, q], ys_r.at[p, q, 2], y=y).start()

    def rs_final(p, q):
        e0, n = span(p, q)
        blk = 3 * n * cap
        at = pl.ds(3 * cap * e0, blk)
        received(fin.at[p, :, at], ys_r.at[p, q, 2])
        total = block(p, q, t)[...].astype(F32) + fin[p, 0, at, :].astype(F32) + fin[p, 1, at, :].astype(F32)
        ysum[p, at, :] = total.astype(BF16)
        sent(part.at[p % 2, pl.ds(12 * cap * e0, 3 * blk)], ys_s.at[p, q])
        send_back(p, q)

    col_a, col_b = pl.ds(0, LANES), pl.ds(LANES, LANES)

    def send_back(p, q):
        e0, n = span(p, q)
        rq = n * cap

        def unit(u):
            return ysum.at[p, pl.ds(pl.multiple_of(3 * cap * e0 + u * rq, rq), rq)]

        def home(col):
            return back.at[me, pl.ds(e0 * cap, rq), col]

        if p == 0:
            back[me, e0 * cap:e0 * cap + rq, 0:LANES] = unit(2 * c)[...]
            rcopy(unit(2 - 2 * c), home(col_a), bk_s.at[0], bk_r.at[me, 0], e=sib).start()
            other = rcopy(unit(1), home(col_b), bk_s.at[1], bk_r.at[me, 1], e=sib)

            @pl.when(has_b)
            def _():
                back[me, e0 * cap:e0 * cap + rq, LANES:2 * LANES] = unit(1)[...]

            @pl.when(jnp.logical_not(has_b))
            def _():
                other.start()
        else:
            je, jo = phases[p]
            jb = je + (t // 2) * (jo - je)
            rcopy(unit(0), home(col_a), bk_s.at[2], bk_r.at[me, 0], e=je).start()
            rcopy(unit(2), home(col_a), bk_s.at[2], bk_r.at[me, 0], e=jo).start()
            rcopy(unit(1), home(col_b), bk_s.at[2], bk_r.at[me, 1], e=jb).start()

    back_chip = (cx, xr + c * (xl - xr), xl + c * (xr - xl), xo)

    def combine(p):
        srcs = (me, sib) if p == 0 else (2 * back_chip[p], 2 * back_chip[p] + 1)
        for m in srcs[1:] if p == 0 else srcs:
            received(back.at[m, :, col_a], bk_r.at[m, 0])

            @pl.when(has_b)
            def _(m=m):
                received(back.at[m, :, col_b], bk_r.at[m, 1])

        def some(i, carry):
            r = pl.ds(pl.multiple_of(i * quart, quart), quart)
            lane = lax.broadcasted_iota(jnp.int32, (quart, rows), 1)
            sums = None
            for m in srcs:
                for q in range(2):
                    pick = jnp.where(lane == meta[r, 2 + q:3 + q] - rows * m, 1.0, 0.0).astype(BF16)
                    term = gate[r, q:q + 1] * jnp.dot(pick, back[m], preferred_element_type=F32)
                    sums = term if sums is None else sums + term
            if p < 3:
                acc[r, :] = sums if p == 0 else acc[r, :] + sums
            else:
                full = (acc[r, :] + sums).astype(BF16)
                outt[ka, r, :] = full[:, :LANES]

                @pl.when(has_b)
                def _():
                    outt[kb, r, :] = full[:, LANES:]
                spread(i)
            return carry
        if p < 3:
            lax.fori_loop(0, n_tok // quart, some, 0)
        else:
            for i in range(n_tok // quart):
                some(i, 0)

    def own_col(y):
        return 2 * y - jnp.where(c == 0, y // (nt - 1), (y + nt - 1) // nt), jnp.clip(jnp.where(c == 0, 2 * y + 1, 2 * y - 2), 0, n_col - 1)

    def owns_b(y):
        return c == y // 2

    ka, kb = own_col(t)

    def col_part(k, i):
        return outt.at[k, pl.ds(i * quart, quart)]

    def store(k, i, cond):
        to_hbm = out_ref.at[pl.ds(i * quart, quart), pl.ds(pl.multiple_of(k * LANES, LANES), LANES)]
        do(cond, pltpu.make_async_copy(col_part(k, i), to_hbm, st_sem).start)

    def do(cond, f):
        if cond is None:
            f()
        else:
            pl.when(cond)(f)

    def col_send(n, k, i, y, cond, sem):
        do(cond, rcopy(col_part(k, i), col_part(k, i), fa_s.at[sem], fa_r.at[n, i], y=y).start)

    def col_recv(n, k, i, cond):
        do(cond, lambda: received(col_part(k, i), fa_r.at[n, i]))
        store(k, i, cond)

    def spread(i):
        for n, k, cond in ((0, ka, None), (1, kb, has_b)):
            col_send(n, k, i, tr, cond, n)
            col_send(2 + n, k, i, tl, cond, n)
            store(k, i, cond)

    def collect():
        (kal, kbl), (kar, kbr), (kao, kbo) = own_col(tl), own_col(tr), own_col(to)
        for i in range(n_tok // quart):
            for n, k, cond in ((0, kal, None), (1, kbl, owns_b(tl))):
                col_recv(n, k, i, cond)
                if i % 2 == 0:
                    col_send(4 + n, k, i, tr, cond, 2 * n)
            for n, k, cond in ((2, kar, None), (3, kbr, owns_b(tr))):
                col_recv(n, k, i, cond)
                if i % 2 == 1:
                    col_send(2 + n, k, i, tl, cond, 3 * (n - 2))
        for i in range(n_tok // quart):
            for n, k, cond in ((4, kao, None), (5, kbo, owns_b(to))):
                col_recv(n, k, i, cond)

    def gates():
        rload.wait()
        w = wr[...]
        hi = w.astype(BF16)
        r1 = w - hi.astype(F32)
        mid = r1.astype(BF16)
        lo = (r1 - mid.astype(F32)).astype(BF16)

        def some(i, carry):
            r = pl.ds(pl.multiple_of(i * quart, quart), quart)
            xs = tok[me, r, :]
            logits = sum(lax.dot_general(xs, v, (((1,), (1,)), ((), ())), preferred_element_type=F32) for v in (lo, mid, hi))
            un = jnp.exp(logits - jnp.max(logits, axis=1, keepdims=True))
            prob = un / jnp.sum(un, axis=1, keepdims=True)
            lane = lax.broadcasted_iota(jnp.int32, (quart, n_exp), 1)
            p1 = jnp.sum(jnp.where(lane == meta[r, 0:1], prob, 0.0), axis=1, keepdims=True)
            p2 = jnp.sum(jnp.where(lane == meta[r, 1:2], prob, 0.0), axis=1, keepdims=True)
            both = p1 + p2
            gate[r, 0:1] = p1 / both
            gate[r, 1:2] = p2 / both
            return carry
        lax.fori_loop(0, n_tok // quart, some, 0)

    def share_out():
        for dr, j in enumerate(pieces(1)):
            mine = share(j, t)
            received(mine, xa_r.at[2 * dr])
            rcopy(mine, mine, ya_s.at[0], ya_r.at[dr, 0], y=tr).start()
            rcopy(mine, mine, ya_s.at[0], ya_r.at[dr, 1], y=tl).start()

    def share_on():
        for dr, j in enumerate(pieces(1)):
            for k, y, far_y in ((0, tl, tr), (1, tr, tl)):
                received(share(j, y), ya_r.at[dr, k])
                on = share(j, y, k)
                rcopy(on, on, ya_s.at[1], ya_r.at[dr, 2 + k], y=far_y).start()

    def arrive(p, step):
        off = quart * (1 - step)
        for dr, j in enumerate(pieces(p)):
            got = piece(j, off, quart)
            if step == 1:
                received(got, xs_r.at[2 * dr + p - 1])
            elif p == 1:
                for k in range(2):
                    received(share(j, to, k), ya_r.at[dr, 2 + k])
            else:
                received(got, xa_r.at[2 * dr + 1])
            if step == 1 - dr:
                rcopy(got, got, xs_s.at[0], xs_r.at[3 + p + 2 * dr], e=2 * (xl if dr else xr) + c).start()
            rcopy(got, got, dd_s, dd_r.at[1 + p], e=sib).start()

    def arrived(p):
        received(tok.at[0], dd_r.at[1 + p])

    far = ((6, 2 * xo + 1, quart), (4, 2 * xo, 0), (5, 2 * xo + 1, 0), (7, 2 * xo, quart))

    def arrive_far(*which):
        for n in which:
            i, j, off = far[n]
            got = piece(j, off, quart)
            received(got, xs_r.at[i])
            rcopy(got, got, dd_s, dd_r.at[4], e=sib).start()

    def arrived_far():
        received(tok.at[0], dd_r.at[4])

    def finish():
        sent(tok.at[pl.ds(0, 4)], dd_s)
        sent(dstb.at[pl.ds(0, ne - 1)], ds_s)
        sent(tok.at[pl.ds(0, 2)], xs_s.at[0])
        sent(tok.at[0, pl.ds(0, 2 * quart // nt)], xs_s.at[1])
        sent(tok.at[0, pl.ds(0, 2 * quart)], xs_s.at[2])
        sent(tok.at[0, pl.ds(0, 4 * quart // nt)], ya_s.at[0])
        sent(tok.at[0, pl.ds(0, 2 * quart // nt)], ya_s.at[1])
        sent(ysum.at[0, pl.ds(0, rows)], bk_s.at[0])
        pl.when(jnp.logical_not(has_b))(lambda: sent(ysum.at[0, pl.ds(0, rows)], bk_s.at[1]))
        sent(ysum.at[pl.ds(0, 3)], bk_s.at[2])
        sent(outt.at[pl.ds(0, 3)], fa_s.at[0])
        pl.when(has_b)(lambda: sent(outt.at[pl.ds(0, 2)], fa_s.at[1]))
        pl.when(owns_b(tl))(lambda: sent(outt.at[0, pl.ds(0, 2 * quart)], fa_s.at[2]))
        pl.when(owns_b(tr))(lambda: sent(outt.at[0, pl.ds(0, 2 * quart)], fa_s.at[3]))
        pltpu.make_async_copy(outt, outt, st_sem).wait()

    plan = [
        (gather_rows, 0, 0), (share_out,), (experts, 0, 0), (rs_start, 0, 0), (gather_rows, 0, 1), (experts, 0, 1), (share_on,), (rs_start, 0, 1),
        (gates,), (rs_mid, 0, 0), (arrive, 1, 0), (arrive, 1, 1), (arrived, 1),
        (gather_rows, 1, 0), (rs_mid, 0, 1), (experts, 1, 0), (rs_start, 1, 0), (gather_rows, 1, 1), (rs_final, 0, 0), (arrive, 2, 0), (experts, 1, 1), (rs_start, 1, 1), (rs_final, 0, 1),
        (arrive, 2, 1), (rs_mid, 1, 0), (arrived, 2),
        (gather_rows, 2, 0), (rs_mid, 1, 1), (experts, 2, 0), (rs_start, 2, 0), (gather_rows, 2, 1), (rs_final, 1, 0), (arrive_far, 0), (experts, 2, 1), (rs_start, 2, 1), (rs_final, 1, 1),
        (combine, 0), (arrive_far, 1), (rs_mid, 2, 0), (arrive_far, 2, 3), (arrived_far,),
    ]
    if len(CHUNKS[3]) == 2:
        plan += [
            (gather_rows, 3, 0), (experts, 3, 0), (rs_start, 3, 0), (rs_mid, 2, 1), (rs_final, 2, 0), (gather_rows, 3, 1), (experts, 3, 1), (rs_start, 3, 1), (rs_final, 2, 1),
            (rs_mid, 3, 0), (combine, 1), (rs_mid, 3, 1), (combine, 2), (rs_final, 3, 0), (rs_final, 3, 1), (combine, 3), (collect,), (finish,),
        ]
    else:
        plan += [
            (gather_rows, 3, 0), (experts, 3, 0), (rs_start, 3, 0), (rs_mid, 2, 1), (rs_final, 2, 0), (gather_rows, 3, 1), (experts, 3, 1), (rs_start, 3, 1),
            (gather_rows, 3, 2), (rs_mid, 3, 0), (experts, 3, 2), (rs_final, 2, 1), (rs_start, 3, 2),
            (combine, 1), (rs_mid, 3, 1), (rs_final, 3, 0), (rs_mid, 3, 2), (combine, 2), (rs_final, 3, 1), (rs_final, 3, 2), (combine, 3), (collect,), (finish,),
        ]
    for f, *at in plan:
        with jax.named_scope(f.__name__ + "".join(str(v) for v in at)):
            f(*at)


def solution(mesh):
    tok_spec = P(("dp", "ep"), None)
    w_in_spec = P("ep", None, "tp")
    w_out_spec = P("ep", "tp", None)
    nt, ne = mesh.shape["tp"], mesh.shape["ep"]

    def local_step(x_tok, w_router, w_gelu, w_lin, w_out, expert_idx, slot_idx):
        n_tok, d = x_tok.shape
        n_exp = w_router.shape[1]
        n_loc, _, f = w_gelu.shape
        cap = 2 * CAP_FACTOR * n_tok // n_exp
        rows = n_loc * cap
        hbm = pl.BlockSpec(memory_space=pl.ANY)
        dma = pltpu.SemaphoreType.DMA
        nq = max(len(v) for v in CHUNKS)
        return pl.pallas_call(
            functools.partial(moe_kernel, nt, ne),
            out_shape=jax.ShapeDtypeStruct((n_tok, d), BF16),
            in_specs=[hbm] * 7,
            out_specs=hbm,
            scratch_shapes=[
                pltpu.VMEM((2, 2, n_tok), jnp.int32),
                pltpu.VMEM((n_tok, 8), jnp.int32),
                pltpu.VMEM((n_exp, d), F32),
                pltpu.VMEM((ne, n_tok, d), BF16),
                pltpu.VMEM((ne, 2, n_tok), jnp.int32),
                pltpu.VMEM((n_loc, 3, d, f), BF16),
                pltpu.VMEM((n_loc, 2 * cap, d), BF16),
                pltpu.VMEM((2, 12 * rows, LANES), BF16),
                pltpu.VMEM((4, 2, 3 * rows // 2, LANES), BF16),
                pltpu.VMEM((4, 2, 3 * rows, LANES), BF16),
                pltpu.VMEM((4, 3 * rows, LANES), BF16),
                pltpu.VMEM((ne, rows, 2 * LANES), BF16),
                pltpu.VMEM((n_tok, 2 * LANES), F32),
                pltpu.VMEM((n_tok, 2), F32),
                pltpu.VMEM((d // LANES, n_tok, LANES), BF16),
                dma((4,)), dma((n_loc,)), dma((3,)), dma((8,)), dma((4,)), dma((2,)), dma((2, 4)), dma, dma((5,)), dma, dma((2,)),
                dma((4, nq)), dma((4, nq, 3)), dma((3,)), dma((ne, 2)), dma((4,)), dma((6, 4)), dma,
            ],
            compiler_params=pltpu.CompilerParams(collective_id=0, has_side_effects=True, vmem_limit_bytes=67043328),
            name="moe",
        )(x_tok, w_router.T, w_gelu, w_lin, w_out, expert_idx.T, slot_idx.T)

    return jax.shard_map(local_step, mesh=mesh, in_specs=(tok_spec, P(), w_in_spec, w_in_spec, w_out_spec, tok_spec, tok_spec), out_specs=tok_spec, check_vma=False)
```

```python
import functools

import jax
import jax.numpy as jnp
from jax import lax
from jax.experimental import pallas as pl
from jax.experimental.pallas import tpu as pltpu
from jax.sharding import PartitionSpec as P

CAP_FACTOR = 2
LANES = 128
MESH = pl.DeviceIdType.MESH
F32 = jnp.float32
BF16 = jnp.bfloat16
UNITS = [(0, 0), (0, 1), (1, 0), (0, 2), (0, 3), (1, 1), (0, 4), (1, 2), (1, 3), (0, 5), (1, 4), (1, 5)]
UNIT_OF = {unit: i for i, unit in enumerate(UNITS)}
SHARED = (256, 128)
CHUNKS = ((4, 4), (4, 4), (4, 4), (3, 3, 2))


def gelu(a):
    return a * (0.5 * (1.0 + jnp.tanh(0.7978845608028654 * (a + 0.044715 * (a * a * a)))))


def moe_kernel(nt, ne, x_hbm, wr_hbm, w0_hbm, w1_hbm, wo_hbm, exp_hbm, slot_hbm, out_ref, route, meta, wr, tok, dstb, wts, xbuf, part, hin, fin, ysum, back, acc,
               gate, outt, ld_sem, w_sem, xs_s, xs_r, xa_r, ya_s, ya_r, dd_s, dd_r, ds_s, ds_r, ys_s, ys_r, bk_s, bk_r, fa_s, fa_r, st_sem):
    n_tok, d = x_hbm.shape
    n_loc = w0_hbm.shape[0]
    n_exp = wr.shape[0]
    cap = 2 * CAP_FACTOR * n_tok // n_exp
    rows = n_loc * cap
    half, quart = n_tok // 2, n_tok // 4
    n_col = d // LANES
    nx = ne // 2
    me, t = lax.axis_index("ep"), lax.axis_index("tp")
    cx, c = me // 2, me % 2
    xr, xl, xo = (cx + 1) % nx, (cx + nx - 1) % nx, (cx + 2) % nx
    sib = me + 1 - 2 * c
    tr, tl, to = (t + 1) % nt, (t + nt - 1) % nt, (t + 2) % nt
    has_b = c == t // 2

    def rcopy(src, dst, s, r, e=None, y=None):
        dev = {"ep": me if e is None else e, "tp": t if y is None else y}
        return pltpu.make_async_remote_copy(src_ref=src, dst_ref=dst, send_sem=s, recv_sem=r, device_id=dev, device_id_type=MESH)

    def received(ref, r):
        rcopy(ref, ref, ds_s, r).wait_recv()

    def sent(ref, s):
        rcopy(ref, ref, s, ds_r.at[0]).wait_send()

    def apart(f):
        pl.when(t >= 0)(f)

    barrier = pltpu.get_barrier_semaphore()
    for k in range(1, ne):
        pl.semaphore_signal(barrier, inc=1, device_id={"ep": (me + k) % ne, "tp": t}, device_id_type=MESH)
    for y in (tr, tl):
        pl.semaphore_signal(barrier, inc=1, device_id={"ep": me, "tp": y}, device_id_type=MESH)
    xload = pltpu.make_async_copy(x_hbm, tok.at[me], ld_sem.at[0])
    eload = pltpu.make_async_copy(exp_hbm, route.at[0], ld_sem.at[1])
    sload = pltpu.make_async_copy(slot_hbm, route.at[1], ld_sem.at[2])
    rload = pltpu.make_async_copy(wr_hbm, wr, ld_sem.at[3])
    eload.start()
    sload.start()
    xload.start()
    eload.wait()
    sload.wait()
    slots = route[1]
    dest = jnp.where(slots >= 0, route[0] * cap + slots - me * cap, -1)
    dstb[me] = dest
    with jax.named_scope("barrier"):
        pl.semaphore_wait(barrier, ne - 1 + 2)
    xload.wait()

    hc = pl.multiple_of(half * c, half)
    hs = pl.multiple_of(half * (1 - c), half)
    give = tok.at[me, pl.ds(hs, half)]
    rcopy(give, give, dd_s, dd_r.at[0], e=sib).start()
    for k in range(1, ne):
        e = (me + k) % ne
        rcopy(dstb.at[me], dstb.at[me], ds_s, ds_r.at[jnp.where(e == sib, 0, 1)], e=e).start()

    def piece(j, off=0, n=half):
        return tok.at[j, pl.ds(pl.multiple_of(hc + off, quart), n)]

    def spiece(j, off=0, n=half):
        return tok.at[j, pl.ds(pl.multiple_of(hs + off, quart), n)]

    def share(p, j, y, h=None):
        n = SHARED[p - 1] // nt
        lo, m = (0, n) if h is None else (h * n // 2, n // 2)
        return tok.at[j, pl.ds(pl.multiple_of(hc + half - SHARED[p - 1] + y * n + lo, 16), m)]

    def alone(p, step):
        n = half - SHARED[p - 1]
        return (0, min(n, quart)) if step else (quart, max(n - quart, 0))

    ev, od = 2 * cx, 2 * cx + 1
    outgoing = []
    for n, (j, x) in enumerate(((ev, xr), (od, xr), (od, xl), (ev, xl))):
        p = 1 + n % 2
        copies = []
        if SHARED[p - 1]:
            copies.append((share(p, j, t), xs_s.at[p], xa_r.at[n]))
        for step in range(2):
            off, m = alone(p, step)
            if m:
                copies.append((piece(j, off, m), xs_s.at[1 + 2 * p + step], xs_r.at[8 * (1 - step) + n]))
        outgoing.append([rcopy(ref, ref, ss, sr, e=2 * x + c) for ref, ss, sr in copies])

    def xsend(n):
        for copy in outgoing[n]:
            copy.start()

    @pl.when(c == 0)
    def _():
        xsend(0)
        received(piece(sib), dd_r.at[0])
        xsend(2)
        xsend(1)
        xsend(3)

    @pl.when(c == 1)
    def _():
        xsend(2)
        received(piece(sib), dd_r.at[0])
        xsend(0)
        xsend(3)
        xsend(1)

    rcopy(piece(me), piece(me), dd_s, dd_r.at[1], e=sib).start()

    def load_weights(e):
        for i, h in enumerate((w0_hbm, w1_hbm, wo_hbm)):
            pltpu.make_async_copy(h.at[e], wts.at[e, i], w_sem.at[e]).start()

    ahead = 4
    for e in range(ahead):
        load_weights(e)
    rload.start()
    meta[...] = jnp.concatenate([route[0], dest, jnp.zeros((4, n_tok), jnp.int32)], axis=0).T

    phases = ((2 * cx, 2 * cx + 1), (2 * xl, 2 * xr + 1), (2 * xr, 2 * xl + 1), (2 * xo, 2 * xo + 1))

    def pieces(p):
        return phases[1] if p == 1 else phases[2][::-1]

    def span(p, q):
        e0 = sum(CHUNKS[p][:q])
        return e0, CHUNKS[p][q]

    def gather_shard(p, q, s, j):
        e0, n = span(p, q)

        def run():
            want = lax.broadcasted_iota(jnp.int32, (n * cap, n_tok), 0) + (e0 * cap + rows * me)
            hit = (dstb[j, 0:1, :] == want) | (dstb[j, 1:2, :] == want)
            pick = jnp.where(hit, 1.0, 0.0).astype(BF16)
            got = jnp.dot(pick, tok[j], preferred_element_type=F32).astype(BF16)
            for i in range(n):
                xbuf[e0 + i, pl.ds(pl.multiple_of(s * cap, cap), cap), :] = got[i * cap:(i + 1) * cap]
        apart(run)

    def gather_rows(p, q):
        if p == 0:
            gather_shard(p, q, c, me)
            if q == 0:
                received(spiece(sib), dd_r.at[1])
                received(dstb.at[0], ds_r.at[0])
            gather_shard(p, q, 1 - c, sib)
            return
        if p == 1 and q == 0:
            received(dstb.at[pl.ds(0, ne - 2)], ds_r.at[1])
        for s, j in enumerate(phases[p]):
            gather_shard(p, q, s, j)

    def experts(p, q):
        e0, n = span(p, q)
        base = 12 * cap * e0
        slot = p % 2

        def ffn(e):
            if p == 0:
                if e + ahead < n_loc:
                    load_weights(e + ahead)
                pltpu.make_async_copy(wts.at[e], wts.at[e], w_sem.at[e]).wait()
            xe = xbuf[e]
            a = jnp.dot(xe, wts[e, 0], preferred_element_type=F32)
            b = jnp.dot(xe, wts[e, 1], preferred_element_type=F32)
            hid = (gelu(a) * b).astype(BF16)
            y = jnp.dot(hid, wts[e, 2], preferred_element_type=F32).astype(BF16)
            for s in range(2):
                for k in range(n_col):
                    at = base + (UNIT_OF[s, k] * n + e - e0) * cap
                    part[slot, at:at + cap, :] = y[s * cap:(s + 1) * cap, k * LANES:(k + 1) * LANES]

        def run():
            for e in range(e0, e0 + n):
                ffn(e)
        apart(run)

    def block(p, q, y, h=None):
        e0, n = span(p, q)
        blk = 3 * n * cap
        lo, m = (0, blk) if h is None else (h * blk // 2, blk // 2)
        return part.at[p % 2, pl.ds(pl.multiple_of(12 * cap * e0 + y * blk + lo, blk // 2), m)]

    def hin_of(p, q, i):
        e0, n = span(p, q)
        return hin.at[p, i, pl.ds(3 * cap * e0 // 2, 3 * cap * n // 2)]

    def fin_of(p, q, i, h):
        e0, n = span(p, q)
        blk = 3 * n * cap
        return fin.at[p, i, pl.ds(3 * cap * e0 + h * blk // 2, blk // 2)]

    def rs_start(p, q):
        for i, src, dst, sem, y in (
            (0, block(p, q, to, 0), hin_of(p, q, 0), ys_r.at[p, q, 0], tr),
            (1, block(p, q, to, 1), hin_of(p, q, 1), ys_r.at[p, q, 1], tl),
            (2, block(p, q, tr, 1), fin_of(p, q, 0, 1), ys_r.at[p, q, 2], tr),
            (3, block(p, q, tl, 0), fin_of(p, q, 1, 0), ys_r.at[p, q, 2], tl),
        ):
            rcopy(src, dst, ys_s.at[p, q], sem, y=y).start()

    def rs_mid(p, q):
        for i, y, h in ((0, tr, 0), (1, tl, 1)):
            received(hin_of(p, q, i), ys_r.at[p, q, i])
            ref = block(p, q, y, h)
            ref[...] = (ref[...].astype(F32) + hin_of(p, q, i)[...].astype(F32)).astype(BF16)
            rcopy(ref, fin_of(p, q, i, h), ys_s.at[p, q], ys_r.at[p, q, 2], y=y).start()

    def rs_final(p, q):
        e0, n = span(p, q)
        blk = 3 * n * cap
        at = pl.ds(3 * cap * e0, blk)
        received(fin.at[p, :, at], ys_r.at[p, q, 2])
        total = block(p, q, t)[...].astype(F32) + fin[p, 0, at, :].astype(F32) + fin[p, 1, at, :].astype(F32)
        ysum[p, at, :] = total.astype(BF16)
        sent(part.at[p % 2, pl.ds(12 * cap * e0, 3 * blk)], ys_s.at[p, q])
        send_back(p, q)

    col_a, col_b = pl.ds(0, LANES), pl.ds(LANES, LANES)

    def send_back(p, q):
        e0, n = span(p, q)
        rq = n * cap

        def unit(u):
            return ysum.at[p, pl.ds(pl.multiple_of(3 * cap * e0 + u * rq, rq), rq)]

        def home(col):
            return back.at[me, pl.ds(e0 * cap, rq), col]

        if p == 0:
            back[me, e0 * cap:e0 * cap + rq, 0:LANES] = unit(2 * c)[...]
            rcopy(unit(2 - 2 * c), home(col_a), bk_s.at[0], bk_r.at[me, 0], e=sib).start()
            other = rcopy(unit(1), home(col_b), bk_s.at[1], bk_r.at[me, 1], e=sib)

            @pl.when(has_b)
            def _():
                back[me, e0 * cap:e0 * cap + rq, LANES:2 * LANES] = unit(1)[...]

            @pl.when(jnp.logical_not(has_b))
            def _():
                other.start()
        else:
            je, jo = phases[p]
            jb = je + (t // 2) * (jo - je)
            rcopy(unit(0), home(col_a), bk_s.at[2], bk_r.at[me, 0], e=je).start()
            rcopy(unit(2), home(col_a), bk_s.at[2], bk_r.at[me, 0], e=jo).start()
            rcopy(unit(1), home(col_b), bk_s.at[2], bk_r.at[me, 1], e=jb).start()

    back_chip = (cx, xr + c * (xl - xr), xl + c * (xr - xl), xo)

    def combine(p):
        srcs = (me, sib) if p == 0 else (2 * back_chip[p], 2 * back_chip[p] + 1)
        for m in srcs[1:] if p == 0 else srcs:
            received(back.at[m, :, col_a], bk_r.at[m, 0])

            @pl.when(has_b)
            def _(m=m):
                received(back.at[m, :, col_b], bk_r.at[m, 1])

        def some(i, carry):
            r = pl.ds(pl.multiple_of(i * quart, quart), quart)
            lane = lax.broadcasted_iota(jnp.int32, (quart, rows), 1)
            sums = None
            for m in srcs:
                for q in range(2):
                    pick = jnp.where(lane == meta[r, 2 + q:3 + q] - rows * m, 1.0, 0.0).astype(BF16)
                    term = gate[r, q:q + 1] * jnp.dot(pick, back[m], preferred_element_type=F32)
                    sums = term if sums is None else sums + term
            if p < 3:
                acc[r, :] = sums if p == 0 else acc[r, :] + sums
            else:
                full = (acc[r, :] + sums).astype(BF16)
                outt[ka, r, :] = full[:, :LANES]

                @pl.when(has_b)
                def _():
                    outt[kb, r, :] = full[:, LANES:]
                spread(i)
            return carry
        if p < 3:
            lax.fori_loop(0, n_tok // quart, some, 0)
        else:
            for i in range(n_tok // quart):
                some(i, 0)

    def own_col(y):
        return 2 * y - jnp.where(c == 0, y // (nt - 1), (y + nt - 1) // nt), jnp.clip(jnp.where(c == 0, 2 * y + 1, 2 * y - 2), 0, n_col - 1)

    def owns_b(y):
        return c == y // 2

    ka, kb = own_col(t)

    def col_part(k, i):
        return outt.at[k, pl.ds(i * quart, quart)]

    def store(k, i, cond):
        to_hbm = out_ref.at[pl.ds(i * quart, quart), pl.ds(pl.multiple_of(k * LANES, LANES), LANES)]
        do(cond, pltpu.make_async_copy(col_part(k, i), to_hbm, st_sem).start)

    def do(cond, f):
        if cond is None:
            f()
        else:
            pl.when(cond)(f)

    def col_send(n, k, i, y, cond, sem):
        do(cond, rcopy(col_part(k, i), col_part(k, i), fa_s.at[sem], fa_r.at[n, i], y=y).start)

    def col_recv(n, k, i, cond):
        do(cond, lambda: received(col_part(k, i), fa_r.at[n, i]))
        store(k, i, cond)

    def spread(i):
        for n, k, cond in ((0, ka, None), (1, kb, has_b)):
            col_send(n, k, i, tr, cond, n)
            col_send(2 + n, k, i, tl, cond, n)
            store(k, i, cond)

    def collect():
        (kal, kbl), (kar, kbr), (kao, kbo) = own_col(tl), own_col(tr), own_col(to)
        for i in range(n_tok // quart):
            for n, k, cond in ((0, kal, None), (1, kbl, owns_b(tl))):
                col_recv(n, k, i, cond)
                if i % 2 == 0:
                    col_send(4 + n, k, i, tr, cond, 2 * n)
            for n, k, cond in ((2, kar, None), (3, kbr, owns_b(tr))):
                col_recv(n, k, i, cond)
                if i % 2 == 1:
                    col_send(2 + n, k, i, tl, cond, 3 * (n - 2))
        for i in range(n_tok // quart):
            for n, k, cond in ((4, kao, None), (5, kbo, owns_b(to))):
                col_recv(n, k, i, cond)

    def gates():
        rload.wait()
        w = wr[...]
        hi = w.astype(BF16)
        r1 = w - hi.astype(F32)
        mid = r1.astype(BF16)
        lo = (r1 - mid.astype(F32)).astype(BF16)

        def some(i, carry):
            r = pl.ds(pl.multiple_of(i * quart, quart), quart)
            xs = tok[me, r, :]
            logits = sum(lax.dot_general(xs, v, (((1,), (1,)), ((), ())), preferred_element_type=F32) for v in (lo, mid, hi))
            un = jnp.exp(logits - jnp.max(logits, axis=1, keepdims=True))
            prob = un / jnp.sum(un, axis=1, keepdims=True)
            lane = lax.broadcasted_iota(jnp.int32, (quart, n_exp), 1)
            p1 = jnp.sum(jnp.where(lane == meta[r, 0:1], prob, 0.0), axis=1, keepdims=True)
            p2 = jnp.sum(jnp.where(lane == meta[r, 1:2], prob, 0.0), axis=1, keepdims=True)
            both = p1 + p2
            gate[r, 0:1] = p1 / both
            gate[r, 1:2] = p2 / both
            return carry
        lax.fori_loop(0, n_tok // quart, some, 0)

    def share_out(p):
        for dr, j in enumerate(pieces(p)):
            mine = share(p, j, t)
            received(mine, xa_r.at[2 * dr + p - 1])
            rcopy(mine, mine, ya_s.at[p - 1, 0], ya_r.at[p - 1, dr, 0], y=tr).start()
            rcopy(mine, mine, ya_s.at[p - 1, 0], ya_r.at[p - 1, dr, 1], y=tl).start()

    def share_on(p):
        for dr, j in enumerate(pieces(p)):
            for k, y, far_y in ((0, tl, tr), (1, tr, tl)):
                received(share(p, j, y), ya_r.at[p - 1, dr, k])
                on = share(p, j, y, k)
                rcopy(on, on, ya_s.at[p - 1, 1], ya_r.at[p - 1, dr, 2 + k], y=far_y).start()

    def arrive(p, step):
        for dr, j in enumerate(pieces(p)):
            got = piece(j, quart * (1 - step), quart)
            off, m = alone(p, step)
            if m:
                received(piece(j, off, m), xs_r.at[8 * (1 - step) + 2 * dr + p - 1])
            if step == 0 and SHARED[p - 1]:
                for k in range(2):
                    received(share(p, j, to, k), ya_r.at[p - 1, dr, 2 + k])
            if step == 1 - dr:
                rcopy(got, got, xs_s.at[0], xs_r.at[3 + p + 2 * dr], e=2 * (xl if dr else xr) + c).start()
            rcopy(got, got, dd_s, dd_r.at[1 + p], e=sib).start()

    def arrived(p):
        received(tok.at[0], dd_r.at[1 + p])

    far = ((6, 2 * xo + 1, quart), (4, 2 * xo, 0), (5, 2 * xo + 1, 0), (7, 2 * xo, quart))

    def arrive_far(*which):
        for n in which:
            i, j, off = far[n]
            got = piece(j, off, quart)
            received(got, xs_r.at[i])
            rcopy(got, got, dd_s, dd_r.at[4], e=sib).start()

    def arrived_far():
        received(tok.at[0], dd_r.at[4])

    def finish():
        sent(tok.at[pl.ds(0, 4)], dd_s)
        sent(dstb.at[pl.ds(0, ne - 1)], ds_s)
        sent(tok.at[0], xs_s.at[0])
        for p in range(1, 3):
            n = SHARED[p - 1]
            if n:
                sent(tok.at[0, pl.ds(0, 2 * n // nt)], xs_s.at[p])
                sent(tok.at[0, pl.ds(0, n)], ya_s.at[p - 1, 0])
                sent(tok.at[0, pl.ds(0, n // 2)], ya_s.at[p - 1, 1])
            for step in range(2):
                if alone(p, step)[1]:
                    sent(tok.at[0, pl.ds(0, 2 * alone(p, step)[1])], xs_s.at[1 + 2 * p + step])
        sent(ysum.at[0, pl.ds(0, rows)], bk_s.at[0])
        pl.when(jnp.logical_not(has_b))(lambda: sent(ysum.at[0, pl.ds(0, rows)], bk_s.at[1]))
        sent(ysum.at[pl.ds(0, 3)], bk_s.at[2])
        sent(outt.at[pl.ds(0, 3)], fa_s.at[0])
        pl.when(has_b)(lambda: sent(outt.at[pl.ds(0, 2)], fa_s.at[1]))
        pl.when(owns_b(tl))(lambda: sent(outt.at[0, pl.ds(0, 2 * quart)], fa_s.at[2]))
        pl.when(owns_b(tr))(lambda: sent(outt.at[0, pl.ds(0, 2 * quart)], fa_s.at[3]))
        pltpu.make_async_copy(outt, outt, st_sem).wait()

    plan = [
        (gather_rows, 0, 0), (share_out, 1), (experts, 0, 0), (rs_start, 0, 0), (gather_rows, 0, 1), (experts, 0, 1), (share_on, 1), (rs_start, 0, 1),
        (gates,), (share_out, 2), (rs_mid, 0, 0), (arrive, 1, 0), (arrive, 1, 1), (arrived, 1),
        (gather_rows, 1, 0), (rs_mid, 0, 1), (experts, 1, 0), (share_on, 2), (rs_start, 1, 0), (gather_rows, 1, 1), (rs_final, 0, 0), (arrive, 2, 0), (experts, 1, 1), (rs_start, 1, 1), (rs_final, 0, 1),
        (arrive, 2, 1), (rs_mid, 1, 0), (arrived, 2),
        (gather_rows, 2, 0), (rs_mid, 1, 1), (experts, 2, 0), (rs_start, 2, 0), (gather_rows, 2, 1), (rs_final, 1, 0), (arrive_far, 0), (experts, 2, 1), (rs_start, 2, 1), (rs_final, 1, 1),
        (combine, 0), (arrive_far, 1), (rs_mid, 2, 0), (arrive_far, 2, 3), (arrived_far,),
    ]
    if len(CHUNKS[3]) == 2:
        plan += [
            (gather_rows, 3, 0), (experts, 3, 0), (rs_start, 3, 0), (rs_mid, 2, 1), (rs_final, 2, 0), (gather_rows, 3, 1), (experts, 3, 1), (rs_start, 3, 1), (rs_final, 2, 1),
            (rs_mid, 3, 0), (combine, 1), (rs_mid, 3, 1), (combine, 2), (rs_final, 3, 0), (rs_final, 3, 1), (combine, 3), (collect,), (finish,),
        ]
    else:
        plan += [
            (gather_rows, 3, 0), (experts, 3, 0), (rs_start, 3, 0), (rs_mid, 2, 1), (rs_final, 2, 0), (gather_rows, 3, 1), (experts, 3, 1), (rs_mid, 3, 0), (rs_start, 3, 1), (gather_rows, 3, 2), (experts, 3, 2), (rs_mid, 3, 1), (rs_start, 3, 2), (rs_final, 3, 0), (rs_final, 2, 1), (combine, 1), (rs_mid, 3, 2), (rs_final, 3, 1), (rs_final, 3, 2), (combine, 2), (combine, 3), (collect,), (finish,),
        ]
    for f, *at in plan:
        with jax.named_scope(f.__name__ + "".join(str(v) for v in at)):
            f(*at)


def solution(mesh):
    tok_spec = P(("dp", "ep"), None)
    w_in_spec = P("ep", None, "tp")
    w_out_spec = P("ep", "tp", None)
    nt, ne = mesh.shape["tp"], mesh.shape["ep"]

    def local_step(x_tok, w_router, w_gelu, w_lin, w_out, expert_idx, slot_idx):
        n_tok, d = x_tok.shape
        n_exp = w_router.shape[1]
        n_loc, _, f = w_gelu.shape
        cap = 2 * CAP_FACTOR * n_tok // n_exp
        rows = n_loc * cap
        hbm = pl.BlockSpec(memory_space=pl.ANY)
        dma = pltpu.SemaphoreType.DMA
        nq = max(len(v) for v in CHUNKS)
        return pl.pallas_call(
            functools.partial(moe_kernel, nt, ne),
            out_shape=jax.ShapeDtypeStruct((n_tok, d), BF16),
            in_specs=[hbm] * 7,
            out_specs=hbm,
            scratch_shapes=[
                pltpu.VMEM((2, 2, n_tok), jnp.int32),
                pltpu.VMEM((n_tok, 8), jnp.int32),
                pltpu.VMEM((n_exp, d), F32),
                pltpu.VMEM((ne, n_tok, d), BF16),
                pltpu.VMEM((ne, 2, n_tok), jnp.int32),
                pltpu.VMEM((n_loc, 3, d, f), BF16),
                pltpu.VMEM((n_loc, 2 * cap, d), BF16),
                pltpu.VMEM((2, 12 * rows, LANES), BF16),
                pltpu.VMEM((4, 2, 3 * rows // 2, LANES), BF16),
                pltpu.VMEM((4, 2, 3 * rows, LANES), BF16),
                pltpu.VMEM((4, 3 * rows, LANES), BF16),
                pltpu.VMEM((ne, rows, 2 * LANES), BF16),
                pltpu.VMEM((n_tok, 2 * LANES), F32),
                pltpu.VMEM((n_tok, 2), F32),
                pltpu.VMEM((d // LANES, n_tok, LANES), BF16),
                dma((4,)), dma((n_loc,)), dma((7,)), dma((12,)), dma((4,)), dma((2, 2)), dma((2, 2, 4)), dma, dma((5,)), dma, dma((2,)),
                dma((4, nq)), dma((4, nq, 3)), dma((3,)), dma((ne, 2)), dma((4,)), dma((6, 4)), dma,
            ],
            compiler_params=pltpu.CompilerParams(collective_id=0, has_side_effects=True, vmem_limit_bytes=67043328),
            name="moe",
        )(x_tok, w_router.T, w_gelu, w_lin, w_out, expert_idx.T, slot_idx.T)

    return jax.shard_map(local_step, mesh=mesh, in_specs=(tok_spec, P(), w_in_spec, w_in_spec, w_out_spec, tok_spec, tok_spec), out_specs=tok_spec, check_vma=False)
```

```python
import functools

import jax
import jax.numpy as jnp
from jax import lax
from jax.experimental import pallas as pl
from jax.experimental.pallas import tpu as pltpu
from jax.sharding import PartitionSpec as P

CAP_FACTOR = 2
LANES = 128
MESH = pl.DeviceIdType.MESH
F32 = jnp.float32
BF16 = jnp.bfloat16
UNITS = [(0, 0), (0, 1), (1, 0), (0, 2), (0, 3), (1, 1), (0, 4), (1, 2), (1, 3), (0, 5), (1, 4), (1, 5)]
UNIT_OF = {unit: i for i, unit in enumerate(UNITS)}
SHARED = (256, 128)
CHUNKS = ((4, 4), (4, 4), (4, 4), (3, 3, 2))


def gelu(a):
    return a * (0.5 * (1.0 + jnp.tanh(0.7978845608028654 * (a + 0.044715 * (a * a * a)))))


def moe_kernel(nt, ne, x_hbm, wr_hbm, w0_hbm, w1_hbm, wo_hbm, exp_hbm, slot_hbm, out_ref, route, meta, wr, tok, dstb, wts, xbuf, part, hin, fin, ysum, back, acc,
               gate, outt, ld_sem, w_sem, xs_s, xs_r, xa_r, ya_s, ya_r, dd_s, dd_r, ds_s, ds_r, ys_s, ys_r, bk_s, bk_r, fa_s, fa_r, st_sem):
    n_tok, d = x_hbm.shape
    n_loc = w0_hbm.shape[0]
    n_exp = wr.shape[0]
    cap = 2 * CAP_FACTOR * n_tok // n_exp
    rows = n_loc * cap
    half, quart = n_tok // 2, n_tok // 4
    n_col = d // LANES
    nx = ne // 2
    me, t = lax.axis_index("ep"), lax.axis_index("tp")
    cx, c = me // 2, me % 2
    xr, xl, xo = (cx + 1) % nx, (cx + nx - 1) % nx, (cx + 2) % nx
    sib = me + 1 - 2 * c
    tr, tl, to = (t + 1) % nt, (t + nt - 1) % nt, (t + 2) % nt
    has_b = c == t // 2

    def rcopy(src, dst, s, r, e=None, y=None):
        dev = {"ep": me if e is None else e, "tp": t if y is None else y}
        return pltpu.make_async_remote_copy(src_ref=src, dst_ref=dst, send_sem=s, recv_sem=r, device_id=dev, device_id_type=MESH)

    def received(ref, r):
        rcopy(ref, ref, ds_s, r).wait_recv()

    def sent(ref, s):
        rcopy(ref, ref, s, ds_r.at[0]).wait_send()

    def apart(f):
        pl.when(t >= 0)(f)

    barrier = pltpu.get_barrier_semaphore()
    for k in range(1, ne):
        pl.semaphore_signal(barrier, inc=1, device_id={"ep": (me + k) % ne, "tp": t}, device_id_type=MESH)
    for y in (tr, tl):
        pl.semaphore_signal(barrier, inc=1, device_id={"ep": me, "tp": y}, device_id_type=MESH)
    xload = pltpu.make_async_copy(x_hbm, tok.at[me], ld_sem.at[0])
    eload = pltpu.make_async_copy(exp_hbm, route.at[0], ld_sem.at[1])
    sload = pltpu.make_async_copy(slot_hbm, route.at[1], ld_sem.at[2])
    rload = pltpu.make_async_copy(wr_hbm, wr, ld_sem.at[3])
    eload.start()
    sload.start()
    xload.start()
    eload.wait()
    sload.wait()
    slots = route[1]
    dest = jnp.where(slots >= 0, route[0] * cap + slots - me * cap, -1)
    dstb[me] = dest
    with jax.named_scope("barrier"):
        pl.semaphore_wait(barrier, ne - 1 + 2)
    xload.wait()

    hc = pl.multiple_of(half * c, half)
    hs = pl.multiple_of(half * (1 - c), half)
    give = tok.at[me, pl.ds(hs, half)]
    rcopy(give, give, dd_s, dd_r.at[0], e=sib).start()
    for k in range(1, ne):
        e = (me + k) % ne
        rcopy(dstb.at[me], dstb.at[me], ds_s, ds_r.at[jnp.where(e == sib, 0, 1)], e=e).start()

    def piece(j, off=0, n=half):
        return tok.at[j, pl.ds(pl.multiple_of(hc + off, quart), n)]

    def spiece(j, off=0, n=half):
        return tok.at[j, pl.ds(pl.multiple_of(hs + off, quart), n)]

    def share(p, j, y, h=None):
        n = SHARED[p - 1] // nt
        lo, m = (0, n) if h is None else (h * n // 2, n // 2)
        return tok.at[j, pl.ds(pl.multiple_of(hc + half - SHARED[p - 1] + y * n + lo, 16), m)]

    def alone(p, step):
        n = half - SHARED[p - 1]
        return (0, min(n, quart)) if step else (quart, max(n - quart, 0))

    ev, od = 2 * cx, 2 * cx + 1
    outgoing = []
    for n, (j, x) in enumerate(((ev, xr), (od, xr), (od, xl), (ev, xl))):
        p = 1 + n % 2
        copies = []
        if SHARED[p - 1]:
            copies.append((share(p, j, t), xs_s.at[p], xa_r.at[n]))
        for step in range(2):
            off, m = alone(p, step)
            if m:
                copies.append((piece(j, off, m), xs_s.at[1 + 2 * p + step], xs_r.at[8 * (1 - step) + n]))
        outgoing.append([rcopy(ref, ref, ss, sr, e=2 * x + c) for ref, ss, sr in copies])

    def xsend(n):
        for copy in outgoing[n]:
            copy.start()

    @pl.when(c == 0)
    def _():
        xsend(0)
        received(piece(sib), dd_r.at[0])
        xsend(2)
        xsend(1)
        xsend(3)

    @pl.when(c == 1)
    def _():
        xsend(2)
        received(piece(sib), dd_r.at[0])
        xsend(0)
        xsend(3)
        xsend(1)

    rcopy(piece(me), piece(me), dd_s, dd_r.at[1], e=sib).start()

    def load_weights(e):
        for i, h in enumerate((w0_hbm, w1_hbm, wo_hbm)):
            pltpu.make_async_copy(h.at[e], wts.at[e, i], w_sem.at[e]).start()

    ahead = 4
    for e in range(ahead):
        load_weights(e)
    rload.start()
    meta[...] = jnp.concatenate([route[0], dest, jnp.zeros((4, n_tok), jnp.int32)], axis=0).T

    phases = ((2 * cx, 2 * cx + 1), (2 * xl, 2 * xr + 1), (2 * xr, 2 * xl + 1), (2 * xo, 2 * xo + 1))

    def pieces(p):
        return phases[1] if p == 1 else phases[2][::-1]

    def span(p, q):
        e0 = sum(CHUNKS[p][:q])
        return e0, CHUNKS[p][q]

    def gather_shard(p, q, s, j):
        e0, n = span(p, q)

        def run():
            want = lax.broadcasted_iota(jnp.int32, (n * cap, n_tok), 0) + (e0 * cap + rows * me)
            hit = (dstb[j, 0:1, :] == want) | (dstb[j, 1:2, :] == want)
            pick = jnp.where(hit, 1.0, 0.0).astype(BF16)
            got = jnp.dot(pick, tok[j], preferred_element_type=F32).astype(BF16)
            for i in range(n):
                xbuf[e0 + i, pl.ds(pl.multiple_of(s * cap, cap), cap), :] = got[i * cap:(i + 1) * cap]
        apart(run)

    def gather_rows(p, q):
        if p == 0:
            gather_shard(p, q, c, me)
            if q == 0:
                received(spiece(sib), dd_r.at[1])
                received(dstb.at[0], ds_r.at[0])
            gather_shard(p, q, 1 - c, sib)
            return
        if p == 1 and q == 0:
            received(dstb.at[pl.ds(0, ne - 2)], ds_r.at[1])
        for s, j in enumerate(phases[p]):
            gather_shard(p, q, s, j)

    def experts(p, q):
        e0, n = span(p, q)
        base = 12 * cap * e0
        slot = p % 2

        def ffn(e):
            if p == 0:
                if e + ahead < n_loc:
                    load_weights(e + ahead)
                pltpu.make_async_copy(wts.at[e], wts.at[e], w_sem.at[e]).wait()
            xe = xbuf[e]
            a = jnp.dot(xe, wts[e, 0], preferred_element_type=F32)
            b = jnp.dot(xe, wts[e, 1], preferred_element_type=F32)
            hid = (gelu(a) * b).astype(BF16)
            y = jnp.dot(hid, wts[e, 2], preferred_element_type=F32).astype(BF16)
            for s in range(2):
                for k in range(n_col):
                    at = base + (UNIT_OF[s, k] * n + e - e0) * cap
                    part[slot, at:at + cap, :] = y[s * cap:(s + 1) * cap, k * LANES:(k + 1) * LANES]

        def run():
            for e in range(e0, e0 + n):
                ffn(e)
        apart(run)

    def block(p, q, y, h=None):
        e0, n = span(p, q)
        blk = 3 * n * cap
        lo, m = (0, blk) if h is None else (h * blk // 2, blk // 2)
        return part.at[p % 2, pl.ds(pl.multiple_of(12 * cap * e0 + y * blk + lo, blk // 2), m)]

    def hin_of(p, q, i):
        e0, n = span(p, q)
        return hin.at[p, i, pl.ds(3 * cap * e0 // 2, 3 * cap * n // 2)]

    def fin_of(p, q, i, h):
        e0, n = span(p, q)
        blk = 3 * n * cap
        return fin.at[p, i, pl.ds(3 * cap * e0 + h * blk // 2, blk // 2)]

    def rs_start(p, q):
        for i, src, dst, sem, y in (
            (0, block(p, q, to, 0), hin_of(p, q, 0), ys_r.at[p, q, 0], tr),
            (1, block(p, q, to, 1), hin_of(p, q, 1), ys_r.at[p, q, 1], tl),
            (2, block(p, q, tr, 1), fin_of(p, q, 0, 1), ys_r.at[p, q, 2], tr),
            (3, block(p, q, tl, 0), fin_of(p, q, 1, 0), ys_r.at[p, q, 2], tl),
        ):
            rcopy(src, dst, ys_s.at[p, q], sem, y=y).start()

    def rs_mid(p, q):
        for i, y, h in ((0, tr, 0), (1, tl, 1)):
            received(hin_of(p, q, i), ys_r.at[p, q, i])
            ref = block(p, q, y, h)
            ref[...] = (ref[...].astype(F32) + hin_of(p, q, i)[...].astype(F32)).astype(BF16)
            rcopy(ref, fin_of(p, q, i, h), ys_s.at[p, q], ys_r.at[p, q, 2], y=y).start()

    def rs_final(p, q):
        e0, n = span(p, q)
        blk = 3 * n * cap
        at = pl.ds(3 * cap * e0, blk)
        received(fin.at[p, :, at], ys_r.at[p, q, 2])
        total = block(p, q, t)[...].astype(F32) + fin[p, 0, at, :].astype(F32) + fin[p, 1, at, :].astype(F32)
        ysum[p, at, :] = total.astype(BF16)
        sent(part.at[p % 2, pl.ds(12 * cap * e0, 3 * blk)], ys_s.at[p, q])
        send_back(p, q)

    col_a, col_b = pl.ds(0, LANES), pl.ds(LANES, LANES)

    def send_back(p, q):
        e0, n = span(p, q)
        rq = n * cap

        def unit(u):
            return ysum.at[p, pl.ds(pl.multiple_of(3 * cap * e0 + u * rq, rq), rq)]

        def home(col):
            return back.at[me, pl.ds(e0 * cap, rq), col]

        if p == 0:
            back[me, e0 * cap:e0 * cap + rq, 0:LANES] = unit(2 * c)[...]
            rcopy(unit(2 - 2 * c), home(col_a), bk_s.at[0], bk_r.at[me, 0], e=sib).start()
            other = rcopy(unit(1), home(col_b), bk_s.at[1], bk_r.at[me, 1], e=sib)

            @pl.when(has_b)
            def _():
                back[me, e0 * cap:e0 * cap + rq, LANES:2 * LANES] = unit(1)[...]

            @pl.when(jnp.logical_not(has_b))
            def _():
                other.start()
        else:
            je, jo = phases[p]
            jb = je + (t // 2) * (jo - je)
            rcopy(unit(0), home(col_a), bk_s.at[2], bk_r.at[me, 0], e=je).start()
            rcopy(unit(2), home(col_a), bk_s.at[2], bk_r.at[me, 0], e=jo).start()
            rcopy(unit(1), home(col_b), bk_s.at[2], bk_r.at[me, 1], e=jb).start()

    back_chip = (cx, xr + c * (xl - xr), xl + c * (xr - xl), xo)

    def combine(p):
        srcs = (me, sib) if p == 0 else (2 * back_chip[p], 2 * back_chip[p] + 1)
        for m in srcs[1:] if p == 0 else srcs:
            received(back.at[m, :, col_a], bk_r.at[m, 0])

            @pl.when(has_b)
            def _(m=m):
                received(back.at[m, :, col_b], bk_r.at[m, 1])

        def some(i, carry):
            r = pl.ds(pl.multiple_of(i * quart, quart), quart)
            lane = lax.broadcasted_iota(jnp.int32, (quart, rows), 1)
            sums = None
            for m in srcs:
                for q in range(2):
                    pick = jnp.where(lane == meta[r, 2 + q:3 + q] - rows * m, 1.0, 0.0).astype(BF16)
                    term = gate[r, q:q + 1] * jnp.dot(pick, back[m], preferred_element_type=F32)
                    sums = term if sums is None else sums + term
            if p < 3:
                acc[r, :] = sums if p == 0 else acc[r, :] + sums
            else:
                full = (acc[r, :] + sums).astype(BF16)
                outt[ka, r, :] = full[:, :LANES]

                @pl.when(has_b)
                def _():
                    outt[kb, r, :] = full[:, LANES:]
                spread(i)
            return carry
        if p < 3:
            lax.fori_loop(0, n_tok // quart, some, 0)
        else:
            for i in range(n_tok // quart):
                some(i, 0)

    def own_col(y):
        return 2 * y - jnp.where(c == 0, y // (nt - 1), (y + nt - 1) // nt), jnp.clip(jnp.where(c == 0, 2 * y + 1, 2 * y - 2), 0, n_col - 1)

    def owns_b(y):
        return c == y // 2

    ka, kb = own_col(t)

    def col_part(k, i):
        return outt.at[k, pl.ds(i * quart, quart)]

    def store(k, i, cond):
        to_hbm = out_ref.at[pl.ds(i * quart, quart), pl.ds(pl.multiple_of(k * LANES, LANES), LANES)]
        do(cond, pltpu.make_async_copy(col_part(k, i), to_hbm, st_sem).start)

    def do(cond, f):
        if cond is None:
            f()
        else:
            pl.when(cond)(f)

    def col_send(n, k, i, y, cond, sem):
        do(cond, rcopy(col_part(k, i), col_part(k, i), fa_s.at[sem], fa_r.at[n, i], y=y).start)

    def col_recv(n, k, i, cond):
        do(cond, lambda: received(col_part(k, i), fa_r.at[n, i]))
        store(k, i, cond)

    def spread(i):
        for n, k, cond in ((0, ka, None), (1, kb, has_b)):
            col_send(n, k, i, tr, cond, n)
            col_send(2 + n, k, i, tl, cond, n)
            store(k, i, cond)

    def collect():
        (kal, kbl), (kar, kbr), (kao, kbo) = own_col(tl), own_col(tr), own_col(to)
        for i in range(n_tok // quart):
            for n, k, cond in ((0, kal, None), (1, kbl, owns_b(tl))):
                col_recv(n, k, i, cond)
                if i % 2 == 0:
                    col_send(4 + n, k, i, tr, cond, 2 * n)
            for n, k, cond in ((2, kar, None), (3, kbr, owns_b(tr))):
                col_recv(n, k, i, cond)
                if i % 2 == 1:
                    col_send(2 + n, k, i, tl, cond, 3 * (n - 2))
        for i in range(n_tok // quart):
            for n, k, cond in ((4, kao, None), (5, kbo, owns_b(to))):
                col_recv(n, k, i, cond)

    def gates():
        rload.wait()
        w = wr[...]
        hi = w.astype(BF16)
        r1 = w - hi.astype(F32)
        mid = r1.astype(BF16)
        lo = (r1 - mid.astype(F32)).astype(BF16)

        def some(i, carry):
            r = pl.ds(pl.multiple_of(i * quart, quart), quart)
            xs = tok[me, r, :]
            logits = sum(lax.dot_general(xs, v, (((1,), (1,)), ((), ())), preferred_element_type=F32) for v in (lo, mid, hi))
            un = jnp.exp(logits - jnp.max(logits, axis=1, keepdims=True))
            prob = un / jnp.sum(un, axis=1, keepdims=True)
            lane = lax.broadcasted_iota(jnp.int32, (quart, n_exp), 1)
            p1 = jnp.sum(jnp.where(lane == meta[r, 0:1], prob, 0.0), axis=1, keepdims=True)
            p2 = jnp.sum(jnp.where(lane == meta[r, 1:2], prob, 0.0), axis=1, keepdims=True)
            both = p1 + p2
            gate[r, 0:1] = p1 / both
            gate[r, 1:2] = p2 / both
            return carry
        lax.fori_loop(0, n_tok // quart, some, 0)

    def share_out(p):
        for dr, j in enumerate(pieces(p)):
            mine = share(p, j, t)
            received(mine, xa_r.at[2 * dr + p - 1])
            rcopy(mine, mine, ya_s.at[p - 1, 0], ya_r.at[p - 1, dr, 0], y=tr).start()
            rcopy(mine, mine, ya_s.at[p - 1, 0], ya_r.at[p - 1, dr, 1], y=tl).start()

    def share_on(p):
        for dr, j in enumerate(pieces(p)):
            for k, y, far_y in ((0, tl, tr), (1, tr, tl)):
                received(share(p, j, y), ya_r.at[p - 1, dr, k])
                on = share(p, j, y, k)
                rcopy(on, on, ya_s.at[p - 1, 1], ya_r.at[p - 1, dr, 2 + k], y=far_y).start()

    def arrive(p, step):
        for dr, j in enumerate(pieces(p)):
            got = piece(j, quart * (1 - step), quart)
            off, m = alone(p, step)
            if m:
                received(piece(j, off, m), xs_r.at[8 * (1 - step) + 2 * dr + p - 1])
            if step == 0 and SHARED[p - 1]:
                for k in range(2):
                    received(share(p, j, to, k), ya_r.at[p - 1, dr, 2 + k])
            if step == 1 - dr:
                rcopy(got, got, xs_s.at[0], xs_r.at[3 + p + 2 * dr], e=2 * (xl if dr else xr) + c).start()
            rcopy(got, got, dd_s, dd_r.at[1 + p], e=sib).start()

    def arrived(p):
        received(tok.at[0], dd_r.at[1 + p])

    far = ((6, 2 * xo + 1, quart), (4, 2 * xo, 0), (5, 2 * xo + 1, 0), (7, 2 * xo, quart))

    def arrive_far(*which):
        for n in which:
            i, j, off = far[n]
            got = piece(j, off, quart)
            received(got, xs_r.at[i])
            rcopy(got, got, dd_s, dd_r.at[4], e=sib).start()

    def arrived_far():
        received(tok.at[0], dd_r.at[4])

    def finish():
        sent(tok.at[pl.ds(0, 4)], dd_s)
        sent(dstb.at[pl.ds(0, ne - 1)], ds_s)
        sent(tok.at[0], xs_s.at[0])
        for p in range(1, 3):
            n = SHARED[p - 1]
            if n:
                sent(tok.at[0, pl.ds(0, 2 * n // nt)], xs_s.at[p])
                sent(tok.at[0, pl.ds(0, n)], ya_s.at[p - 1, 0])
                sent(tok.at[0, pl.ds(0, n // 2)], ya_s.at[p - 1, 1])
            for step in range(2):
                if alone(p, step)[1]:
                    sent(tok.at[0, pl.ds(0, 2 * alone(p, step)[1])], xs_s.at[1 + 2 * p + step])
        sent(ysum.at[0, pl.ds(0, rows)], bk_s.at[0])
        pl.when(jnp.logical_not(has_b))(lambda: sent(ysum.at[0, pl.ds(0, rows)], bk_s.at[1]))
        sent(ysum.at[pl.ds(0, 3)], bk_s.at[2])
        sent(outt.at[pl.ds(0, 3)], fa_s.at[0])
        pl.when(has_b)(lambda: sent(outt.at[pl.ds(0, 2)], fa_s.at[1]))
        pl.when(owns_b(tl))(lambda: sent(outt.at[0, pl.ds(0, 2 * quart)], fa_s.at[2]))
        pl.when(owns_b(tr))(lambda: sent(outt.at[0, pl.ds(0, 2 * quart)], fa_s.at[3]))
        pltpu.make_async_copy(outt, outt, st_sem).wait()

    plan = [
        (gather_rows, 0, 0), (share_out, 1), (experts, 0, 0), (rs_start, 0, 0), (gather_rows, 0, 1), (experts, 0, 1), (share_on, 1), (rs_start, 0, 1),
        (gates,), (share_out, 2), (rs_mid, 0, 0), (arrive, 1, 0), (arrive, 1, 1), (arrived, 1),
        (gather_rows, 1, 0), (rs_mid, 0, 1), (experts, 1, 0), (share_on, 2), (rs_start, 1, 0), (gather_rows, 1, 1), (rs_final, 0, 0), (arrive, 2, 0), (experts, 1, 1), (rs_start, 1, 1), (rs_final, 0, 1),
        (arrive, 2, 1), (rs_mid, 1, 0), (arrived, 2),
        (gather_rows, 2, 0), (rs_mid, 1, 1), (experts, 2, 0), (rs_start, 2, 0), (gather_rows, 2, 1), (rs_final, 1, 0), (arrive_far, 0), (experts, 2, 1), (rs_start, 2, 1), (rs_final, 1, 1),
        (rs_mid, 2, 0), (arrive_far, 1), (arrive_far, 2, 3), (combine, 0), (arrived_far,),
    ]
    if len(CHUNKS[3]) == 2:
        plan += [
            (gather_rows, 3, 0), (experts, 3, 0), (rs_start, 3, 0), (rs_mid, 2, 1), (rs_final, 2, 0), (gather_rows, 3, 1), (experts, 3, 1), (rs_start, 3, 1), (rs_final, 2, 1),
            (rs_mid, 3, 0), (combine, 1), (rs_mid, 3, 1), (combine, 2), (rs_final, 3, 0), (rs_final, 3, 1), (combine, 3), (collect,), (finish,),
        ]
    else:
        plan += [
(gather_rows, 3, 0), (rs_mid, 2, 1), (experts, 3, 0), (rs_start, 3, 0), (rs_final, 2, 0), (gather_rows, 3, 1), (experts, 3, 1), (rs_mid, 3, 0), (rs_start, 3, 1), (gather_rows, 3, 2), (experts, 3, 2), (rs_final, 2, 1), (rs_start, 3, 2), (rs_mid, 3, 1), (rs_final, 3, 0), (combine, 1), (rs_mid, 3, 2), (rs_final, 3, 1), (rs_final, 3, 2), (combine, 2), (combine, 3), (collect,), (finish,),
        ]
    for f, *at in plan:
        with jax.named_scope(f.__name__ + "".join(str(v) for v in at)):
            f(*at)


def solution(mesh):
    tok_spec = P(("dp", "ep"), None)
    w_in_spec = P("ep", None, "tp")
    w_out_spec = P("ep", "tp", None)
    nt, ne = mesh.shape["tp"], mesh.shape["ep"]

    def local_step(x_tok, w_router, w_gelu, w_lin, w_out, expert_idx, slot_idx):
        n_tok, d = x_tok.shape
        n_exp = w_router.shape[1]
        n_loc, _, f = w_gelu.shape
        cap = 2 * CAP_FACTOR * n_tok // n_exp
        rows = n_loc * cap
        hbm = pl.BlockSpec(memory_space=pl.ANY)
        dma = pltpu.SemaphoreType.DMA
        nq = max(len(v) for v in CHUNKS)
        return pl.pallas_call(
            functools.partial(moe_kernel, nt, ne),
            out_shape=jax.ShapeDtypeStruct((n_tok, d), BF16),
            in_specs=[hbm] * 7,
            out_specs=hbm,
            scratch_shapes=[
                pltpu.VMEM((2, 2, n_tok), jnp.int32),
                pltpu.VMEM((n_tok, 8), jnp.int32),
                pltpu.VMEM((n_exp, d), F32),
                pltpu.VMEM((ne, n_tok, d), BF16),
                pltpu.VMEM((ne, 2, n_tok), jnp.int32),
                pltpu.VMEM((n_loc, 3, d, f), BF16),
                pltpu.VMEM((n_loc, 2 * cap, d), BF16),
                pltpu.VMEM((2, 12 * rows, LANES), BF16),
                pltpu.VMEM((4, 2, 3 * rows // 2, LANES), BF16),
                pltpu.VMEM((4, 2, 3 * rows, LANES), BF16),
                pltpu.VMEM((4, 3 * rows, LANES), BF16),
                pltpu.VMEM((ne, rows, 2 * LANES), BF16),
                pltpu.VMEM((n_tok, 2 * LANES), F32),
                pltpu.VMEM((n_tok, 2), F32),
                pltpu.VMEM((d // LANES, n_tok, LANES), BF16),
                dma((4,)), dma((n_loc,)), dma((7,)), dma((12,)), dma((4,)), dma((2, 2)), dma((2, 2, 4)), dma, dma((5,)), dma, dma((2,)),
                dma((4, nq)), dma((4, nq, 3)), dma((3,)), dma((ne, 2)), dma((4,)), dma((6, 4)), dma,
            ],
            compiler_params=pltpu.CompilerParams(collective_id=0, has_side_effects=True, vmem_limit_bytes=67043328),
            name="moe",
        )(x_tok, w_router.T, w_gelu, w_lin, w_out, expert_idx.T, slot_idx.T)

    return jax.shard_map(local_step, mesh=mesh, in_specs=(tok_spec, P(), w_in_spec, w_in_spec, w_out_spec, tok_spec, tok_spec), out_specs=tok_spec, check_vma=False)
```
